16 devices in a mesh: dp: 4 (over z, y), tp: 4 (over x, core).
Axes of the slice: x: 2, y: 2, z: 2, core: 2. Of those that a mesh axis runs over, the one named last changes fastest.
Arguments:
- hidden: bfloat16 [4, 128, 4096], P('dp'), parts along dimension 0
- ln_gain: float32 [4096], replicated
- ln_bias: float32 [4096], replicated
- embedding: bfloat16 [50688, 4096], P('tp')
- targets: int32 [4, 128], P('dp'), parts along dimension 0
- score_mask: int32 [4, 128], P('dp'), parts along dimension 0
Outputs:
- output 1: float32 [4, 128], P('dp'), parts along dimension 0
- output 2: float32 [4, 128], P('dp'), parts along dimension 0
- output 3: float32 [4], P('dp'), parts along dimension 0
- output 4: float32 [4, 128], P('dp'), parts along dimension 0
There are 4 independent parts. The reference program is written for one: setup_inputs(seed, part) draws one part's arguments, and reference() takes and returns one part's arrays. A program takes and returns all parts, laid end to end along the dimension named above; an argument that names none is the same for every part.
All inputs are finite; a program needn't handle non-finite values.
Results may differ from the reference program's by a relative error of at most 0.001.
Values sent between devices are 32-bit elements.
A program may use at most 1 GiB of HBM per device.

```python
import jax
import jax.numpy as jnp
from jax import lax

BATCH = 1
SEQ_LEN = 128
D_MODEL = 4096
VOCAB = 50272
VOCAB_PAD = 50688
LN_EPS = 1e-5
LOGIT_SCALE = 3.0


def setup_inputs(seed: int = 0, part: int = 0) -> dict:
    part_key = jax.random.fold_in(jax.random.key(seed), part)
    shared_key = jax.random.key(seed + 1)
    key_x, key_tgt, key_lo, key_hi = jax.random.split(part_key, 4)
    key_g, key_b, key_e = jax.random.split(shared_key, 3)
    hidden = jax.random.normal(key_x, (BATCH, SEQ_LEN, D_MODEL), jnp.float32).astype(jnp.bfloat16)
    ln_gain = 1.0 + 0.3 * jax.random.normal(key_g, (D_MODEL,), jnp.float32)
    ln_bias = 0.5 * jax.random.normal(key_b, (D_MODEL,), jnp.float32)
    embedding = (jax.random.normal(key_e, (VOCAB_PAD, D_MODEL), jnp.float32) * (LOGIT_SCALE * D_MODEL ** -0.5)).astype(jnp.bfloat16)
    targets = jax.random.randint(key_tgt, (BATCH, SEQ_LEN), 0, VOCAB, jnp.int32)
    targets = targets.at[0, 0].set(0).at[0, SEQ_LEN - 1].set(VOCAB - 1)
    positions = jnp.arange(SEQ_LEN)[None, :]
    run_start = jax.random.randint(key_lo, (BATCH, 1), 0, SEQ_LEN // 2, jnp.int32)
    run_stop = jax.random.randint(key_hi, (BATCH, 1), SEQ_LEN // 2 + 1, SEQ_LEN + 1, jnp.int32)
    score_mask = ((positions >= run_start) & (positions < run_stop)).astype(jnp.int32)
    return {"hidden": hidden, "ln_gain": ln_gain, "ln_bias": ln_bias, "embedding": embedding, "targets": targets, "score_mask": score_mask}


def reference(hidden, ln_gain, ln_bias, embedding, targets, score_mask):
    vocab_ids = jnp.arange(VOCAB_PAD)
    valid_rows = vocab_ids < VOCAB

    def score_row(row):
        hidden_row, target_row, mask_row = row
        hidden_f = hidden_row.astype(jnp.float32)
        row_mean = jnp.mean(hidden_f, axis=-1, keepdims=True)
        centered = hidden_f - row_mean
        row_var = jnp.mean(centered * centered, axis=-1, keepdims=True)
        normed = (centered * lax.rsqrt(row_var + LN_EPS) * ln_gain + ln_bias).astype(jnp.bfloat16)
        logits = jnp.dot(normed, embedding.T, preferred_element_type=jnp.float32)
        logits = jnp.where(valid_rows[None, :], logits, -jnp.inf)
        row_max = jnp.max(logits, axis=-1)
        log_norm = row_max + jnp.log(jnp.sum(jnp.exp(logits - row_max[:, None]), axis=-1))
        target_logit = jnp.sum(jnp.where(vocab_ids[None, :] == target_row[:, None], logits, 0.0), axis=-1)
        token_logp = (target_logit - log_norm) * mask_row.astype(jnp.float32)
        return log_norm, token_logp, jnp.sum(token_logp), row_max - log_norm

    log_norm, token_logp, seq_score, top_logp = lax.map(score_row, (hidden, targets, score_mask))
    return log_norm, token_logp, seq_score, top_logp
```

```python
import functools

import jax
import jax.numpy as jnp
from jax import lax
from jax.experimental import pallas as pl
from jax.experimental.pallas import tpu as pltpu
from jax.sharding import PartitionSpec as P

OPT_VOCAB = 50272
LN_EPS = 1e-5
BLOCK = 384
SLOTS = 6
MESH = pl.DeviceIdType.MESH
NEG_INF = float("-inf")


def kernel(n_tp, x_hbm, gain_ref, bias_ref, emb_hbm, tgt_ref, msk_ref,
           norm_ref, logp_ref, top_ref, seq_ref,
           x_buf, h_buf, e_buf, m_acc, s_acc, t_acc, send_buf, recv_buf,
           x_sem, e_sem, send_sem, recv_sem):
    dp, tp = lax.axis_index("dp"), lax.axis_index("tp")
    rows = emb_hbm.shape[0]
    tokens = x_buf.shape[0]
    n_blocks = rows // BLOCK
    first_row = tp * rows

    def fetch(i, slot):
        return pltpu.make_async_copy(emb_hbm.at[pl.ds(i * BLOCK, BLOCK)], e_buf.at[slot], e_sem.at[slot])

    x_copy = pltpu.make_async_copy(x_hbm.at[0], x_buf, x_sem)
    x_copy.start()
    for s in range(SLOTS):
        fetch(s, s).start()

    barrier = pltpu.get_barrier_semaphore()
    for k in range(1, n_tp):
        pl.semaphore_signal(barrier, inc=1, device_id={"dp": dp, "tp": lax.rem(tp + k, n_tp)}, device_id_type=MESH)

    x_copy.wait()
    gain, bias = gain_ref[...], bias_ref[...]

    def norm_rows(r, carry):
        sl = pl.ds(pl.multiple_of(r * 16, 16), 16)
        x = x_buf[sl, :].astype(jnp.float32)
        mean = jnp.mean(x, axis=-1, keepdims=True)
        c = x - mean
        var = jnp.mean(c * c, axis=-1, keepdims=True)
        h_buf[sl, :] = (c * lax.rsqrt(var + LN_EPS) * gain + bias).astype(jnp.bfloat16)
        return carry

    lax.fori_loop(0, tokens // 16, norm_rows, 0)

    m_acc[...] = jnp.full_like(m_acc, NEG_INF)
    s_acc[...] = jnp.zeros_like(s_acc)
    t_acc[...] = jnp.zeros_like(t_acc)
    target = tgt_ref[...] - first_row

    def consume(i, masked):
        slot = lax.rem(i, SLOTS)
        fetch(i, slot).wait()
        z = lax.dot_general(e_buf[slot], h_buf[...], (((1,), (1,)), ((), ())), preferred_element_type=jnp.float32)
        z = z.reshape(BLOCK // 8, 8, tokens)
        row = (lax.broadcasted_iota(jnp.int32, z.shape, 0) * 8 + lax.broadcasted_iota(jnp.int32, z.shape, 1)) + i * BLOCK
        if masked:
            z = jnp.where(row < OPT_VOCAB - first_row, z, NEG_INF)
        t_acc[...] += jnp.sum(jnp.where(row == target[None], z, 0.0), axis=0)
        m_old = m_acc[...]
        m_new = jnp.maximum(m_old, jnp.max(z, axis=0))
        safe = jnp.where(m_new == NEG_INF, 0.0, m_new) if masked else m_new
        s_acc[...] = s_acc[...] * jnp.exp(m_old - safe) + jnp.sum(jnp.exp(z - safe[None]), axis=0)
        m_acc[...] = m_new

    n_plain = (rows - 768) // BLOCK

    def step(i, carry):
        consume(i, False)

        @pl.when(i + SLOTS < n_blocks)
        def _():
            fetch(i + SLOTS, lax.rem(i, SLOTS)).start()
        return carry

    lax.fori_loop(0, n_plain, step, 0)

    def last(i, carry):
        consume(i, True)
        return carry
    lax.fori_loop(n_plain, n_blocks, last, 0)

    m8 = m_acc[...]
    m1 = jnp.max(m8, axis=0, keepdims=True)
    s1 = jnp.sum(s_acc[...] * jnp.exp(m8 - m1), axis=0, keepdims=True)
    t1 = jnp.sum(t_acc[...], axis=0, keepdims=True)
    send_buf[0:1, :] = m1
    send_buf[1:2, :] = s1
    send_buf[2:3, :] = t1
    pl.semaphore_wait(barrier, n_tp - 1)
    copies = []
    for k in range(1, n_tp):
        copies.append(pltpu.make_async_remote_copy(
            src_ref=send_buf, dst_ref=recv_buf.at[k - 1], send_sem=send_sem.at[k - 1], recv_sem=recv_sem.at[k - 1],
            device_id={"dp": dp, "tp": lax.rem(tp + k, n_tp)}, device_id_type=MESH))
    for c in copies:
        c.start()
    for c in copies:
        c.wait_recv()
    ms, ss, ts = [m1], [s1], [t1]
    for k in range(1, n_tp):
        ms.append(recv_buf[k - 1, 0:1, :])
        ss.append(recv_buf[k - 1, 1:2, :])
        ts.append(recv_buf[k - 1, 2:3, :])
    m = functools.reduce(jnp.maximum, ms)
    total = sum(s * jnp.exp(mm - m) for s, mm in zip(ss, ms))
    z_t = sum(ts)
    norm = m + jnp.log(total)
    logp = (z_t - norm) * msk_ref[...].astype(jnp.float32)
    norm_ref[...] = norm
    logp_ref[...] = logp
    top_ref[...] = m - norm
    seq_ref[...] = jnp.broadcast_to(jnp.sum(logp, axis=-1, keepdims=True), logp.shape)
    for c in copies:
        c.wait_send()


def solution(mesh):
    n_tp = mesh.shape["tp"]

    def local_part(hidden, ln_gain, ln_bias, embedding, targets, score_mask):
        _, tokens, width = hidden.shape
        row = jax.ShapeDtypeStruct((1, tokens), jnp.float32)
        vmem = pl.BlockSpec(memory_space=pltpu.VMEM)
        hbm = pl.BlockSpec(memory_space=pl.ANY)
        norm, logp, top, seq = pl.pallas_call(
            functools.partial(kernel, n_tp),
            out_shape=(row, row, row, row),
            in_specs=[hbm, vmem, vmem, hbm, vmem, vmem],
            out_specs=(vmem, vmem, vmem, vmem),
            scratch_shapes=[
                pltpu.VMEM((tokens, width), jnp.bfloat16),
                pltpu.VMEM((tokens, width), jnp.bfloat16),
                pltpu.VMEM((SLOTS, BLOCK, width), jnp.bfloat16),
                pltpu.VMEM((8, tokens), jnp.float32),
                pltpu.VMEM((8, tokens), jnp.float32),
                pltpu.VMEM((8, tokens), jnp.float32),
                pltpu.VMEM((8, tokens), jnp.float32),
                pltpu.VMEM((n_tp - 1, 8, tokens), jnp.float32),
                pltpu.SemaphoreType.DMA,
                pltpu.SemaphoreType.DMA((SLOTS,)),
                pltpu.SemaphoreType.DMA((n_tp - 1,)),
                pltpu.SemaphoreType.DMA((n_tp - 1,)),
            ],
            compiler_params=pltpu.CompilerParams(collective_id=0, has_side_effects=True, vmem_limit_bytes=60 << 20),
        )(hidden, ln_gain.reshape(1, width), ln_bias.reshape(1, width), embedding, targets, score_mask)
        return norm, logp, seq[0, :1], top

    row_spec = P("dp", None)
    return jax.shard_map(local_part, mesh=mesh, in_specs=(P("dp", None, None), P(), P(), P("tp", None), row_spec, row_spec), out_specs=(row_spec, row_spec, P("dp"), row_spec), check_vma=False)
```

```python
import functools

import jax
import jax.numpy as jnp
from jax import lax
from jax.experimental import pallas as pl
from jax.experimental.pallas import tpu as pltpu
from jax.sharding import PartitionSpec as P

OPT_VOCAB = 50272
LN_EPS = 1e-5
CHUNK = 512
SHARED = 5632
MESH = pl.DeviceIdType.MESH
NEG_INF = float("-inf")
NT = (((1,), (1,)), ((), ()))


def kernel(n_tp, x_hbm, gain_ref, bias_ref, emb_hbm, tgt_ref, msk_ref, out_ref,
           x_buf, h_buf, hs_buf, fr_buf, e_buf, z_buf, zs_buf, tg_send, tg_recv, own_send, far_send, own_recv, y_recv, z_recv,
           x_sem, s_sem, e_sem, hs_sem, hr_sem, rs_sem, rr_sem, ts_sem, tr_sem, ss_sem, sr_sem):
    dp, tp = lax.axis_index("dp"), lax.axis_index("tp")
    rows, width = emb_hbm.shape
    tokens = x_buf.shape[0]
    half = tokens // 2
    n_chunks = width // CHUNK
    single = rows - 2 * SHARED
    per_slot = SHARED // single
    first_single = n_chunks - pl.cdiv(n_chunks, per_slot)
    core, y, z = tp % 2, dp % 2, dp // 2
    parity = (y + z) % 2
    dp_y, dp_z = dp + 1 - 2 * y, dp + 2 - 4 * z
    dp_far = dp_y + core * (dp_z - dp_y)
    tp_other = tp + 1 - 2 * core
    first_row = tp * rows
    shared_row = pl.multiple_of(parity * SHARED, 16)
    mine = pl.ds(pl.multiple_of(core * half, half), half)

    def fetch_x():
        return pltpu.make_async_copy(x_hbm.at[0], x_buf, x_sem)

    def fetch_single(c):
        src = emb_hbm.at[pl.ds(2 * SHARED, single), pl.ds(pl.multiple_of(c * CHUNK, CHUNK), CHUNK)]
        return pltpu.make_async_copy(src, single_ref(c), s_sem.at[c])

    def single_ref(c):
        return e_buf.at[first_single + c // per_slot, pl.ds(pl.multiple_of(c % per_slot * single, 16), single)]

    def fetch_shared(c):
        src = emb_hbm.at[pl.ds(shared_row, SHARED), pl.ds(pl.multiple_of(c * CHUNK, CHUNK), CHUNK)]
        return pltpu.make_async_copy(src, e_buf.at[c], e_sem.at[c])

    def send_h(c):
        return pltpu.make_async_remote_copy(hs_buf.at[c], fr_buf.at[c, mine], hs_sem.at[c], hr_sem.at[c], device_id={"dp": dp_far, "tp": tp}, device_id_type=MESH)

    def relay_h(c):
        return pltpu.make_async_remote_copy(fr_buf.at[c, mine], fr_buf.at[c, mine], rs_sem.at[c], rr_sem.at[c], device_id={"dp": dp, "tp": tp_other}, device_id_type=MESH)

    def send_targets(k):
        to = tp if k == 0 else tp_other
        return pltpu.make_async_remote_copy(tg_send, tg_recv.at[core], ts_sem.at[k], tr_sem.at[core], device_id={"dp": dp_far, "tp": to}, device_id_type=MESH)

    fetch_x().start()
    for c in range(n_chunks):
        fetch_single(c).start()
    for c in range(first_single):
        fetch_shared(c).start()

    barrier = pltpu.get_barrier_semaphore()
    group = [(dp, k) for k in range(1, n_tp)] + [(dp_y, k) for k in range(n_tp)] + [(dp_z, k) for k in range(n_tp)]
    for d, k in group:
        pl.semaphore_signal(barrier, inc=1, device_id={"dp": d, "tp": (tp + k) % n_tp}, device_id_type=MESH)
    tg_send[...] = jnp.broadcast_to(tgt_ref[...].astype(jnp.float32), tg_send.shape)

    def clear(i, carry):
        z_buf[pl.ds(pl.multiple_of(i * 64, 64), 64), :] = jnp.zeros((64, 2 * tokens), jnp.float32)
        return carry

    lax.fori_loop(0, SHARED // 64, clear, 0)
    zs_buf[...] = jnp.zeros_like(zs_buf)

    fetch_x().wait()

    def norm_rows(row):
        sl = pl.ds(pl.multiple_of(row, 16), 16)
        x = x_buf[sl, :].astype(jnp.float32)
        mean = jnp.mean(x, axis=-1, keepdims=True)
        c = x - mean
        var = jnp.mean(c * c, axis=-1, keepdims=True)
        h = (c * lax.rsqrt(var + LN_EPS) * gain_ref[...] + bias_ref[...]).astype(jnp.bfloat16)
        for k in range(n_chunks):
            h_buf[k, sl, :] = h[:, k * CHUNK:(k + 1) * CHUNK]
        return h

    def norm_sent(g, carry):
        h = norm_rows(core * half + g * 16).astype(jnp.float32)
        for k in range(n_chunks):
            hs_buf[k, pl.ds(pl.multiple_of(g * 16, 16), 16), :] = h[:, k * CHUNK:(k + 1) * CHUNK]
        return carry

    def norm_kept(g, carry):
        norm_rows((1 - core) * half + g * 16)
        return carry

    lax.fori_loop(0, half // 16, norm_sent, 0)
    pl.semaphore_wait(barrier, len(group))
    for c in range(n_chunks):
        send_h(c).start()
    for k in range(2):
        send_targets(k).start()
    lax.fori_loop(0, half // 16, norm_kept, 0)

    def single_chunk(c, carry):
        fetch_single(c).wait()
        zs_buf[...] += lax.dot_general(single_ref(c)[...], h_buf[c, 0:tokens, :], NT, preferred_element_type=jnp.float32)
        return carry

    lax.fori_loop(0, n_chunks, single_chunk, 0)
    for c in range(first_single, n_chunks):
        fetch_shared(c).start()

    def row_ids(block, start):
        shape = (block // 8, 8, 1)
        return lax.broadcasted_iota(jnp.int32, shape, 0) * 8 + lax.broadcasted_iota(jnp.int32, shape, 1) + start

    def stats(z_ref, n_rows, block, start, target, limit):
        lanes = z_ref.shape[1]

        def load(i):
            zz = z_ref[pl.ds(pl.multiple_of(i * block, block), block), :].reshape(block // 8, 8, lanes)
            ids = row_ids(block, start + i * block)
            if limit is not None:
                zz = jnp.where(ids < limit, zz, NEG_INF)
            return zz, ids

        def top(i, carry):
            m8, t8 = carry
            zz, ids = load(i)
            return jnp.maximum(m8, jnp.max(zz, axis=0)), t8 + jnp.sum(jnp.where(ids == target[None], zz, 0.0), axis=0)

        m8, t8 = lax.fori_loop(0, n_rows // block, top, (jnp.full((8, lanes), NEG_INF), jnp.zeros((8, lanes), jnp.float32)))
        m1 = jnp.max(m8, axis=0, keepdims=True)

        def add(i, s8):
            zz, _ = load(i)
            return s8 + jnp.sum(jnp.exp(zz - m1[None]), axis=0)

        s8 = lax.fori_loop(0, n_rows // block, add, jnp.zeros((8, lanes), jnp.float32))
        return m1, jnp.sum(s8, axis=0, keepdims=True), jnp.sum(t8, axis=0, keepdims=True)

    target = tgt_ref[...]
    m_s, s_s, t_s = stats(zs_buf, single, 128, first_row + 2 * SHARED, target, OPT_VOCAB)

    send_h(0).wait_recv()
    relay_h(0).start()

    def shared_chunk(c, carry):
        @pl.when(c + 1 < n_chunks)
        def _():
            send_h(c + 1).wait_recv()
            relay_h(c + 1).start()
        relay_h(c).wait_recv()
        h_buf[c, tokens:2 * tokens, :] = fr_buf[c].astype(jnp.bfloat16)
        fetch_shared(c).wait()
        z_buf[...] += lax.dot_general(e_buf[c], h_buf[c], NT, preferred_element_type=jnp.float32)
        return carry

    lax.fori_loop(0, n_chunks, shared_chunk, 0)

    for k in range(2):
        pltpu.make_async_remote_copy(tg_send, tg_recv.at[k], ts_sem.at[k], tr_sem.at[k], device_id={"dp": dp_far, "tp": tp}, device_id_type=MESH).wait_recv()
    lane = lax.broadcasted_iota(jnp.int32, (1, tokens), 1)
    far_target = jnp.where(lane < half, tg_recv[0, 0:1, :], tg_recv[1, 0:1, :]).astype(jnp.int32)
    both = jnp.concatenate([target, far_target], axis=1)
    m_h, s_h, t_h = stats(z_buf, SHARED, 128, first_row + shared_row, both, None)

    m_o = jnp.maximum(m_s, m_h[:, :tokens])
    s_o = s_s * jnp.exp(m_s - m_o) + s_h[:, :tokens] * jnp.exp(m_h[:, :tokens] - m_o)
    t_o = t_s + t_h[:, :tokens]
    own_send[0:1, :] = m_o
    own_send[1:2, :] = s_o
    own_send[2:3, :] = t_o
    far_send[0:1, :] = m_h[:, tokens:]
    far_send[1:2, :] = s_h[:, tokens:]
    far_send[2:3, :] = t_h[:, tokens:]

    copies = []
    for i, (d, k) in enumerate(group):
        src = own_send if i < n_tp - 1 else far_send
        dst = own_recv.at[k - 1] if i < n_tp - 1 else (y_recv.at[k] if i < 2 * n_tp - 1 else z_recv.at[k])
        copies.append(pltpu.make_async_remote_copy(src, dst, ss_sem.at[i], sr_sem.at[i], device_id={"dp": d, "tp": (tp + k) % n_tp}, device_id_type=MESH))
    for c in copies:
        c.start()
    for c in range(n_chunks):
        send_h(c).wait_send()
        relay_h(c).wait_send()
    for k in range(2):
        send_targets(k).wait_send()
    for c in copies:
        c.wait_recv()

    parts = [(m_o, s_o, t_o)]
    for k in range(n_tp - 1):
        parts.append(tuple(own_recv[k, j:j + 1, :] for j in range(3)))
    for k in range(n_tp):
        parts.append(tuple(jnp.where(lane < half, y_recv[k, j:j + 1, :], z_recv[k, j:j + 1, :]) for j in range(3)))
    m = functools.reduce(jnp.maximum, [p[0] for p in parts])
    total = sum(p[1] * jnp.exp(p[0] - m) for p in parts)
    z_t = sum(p[2] for p in parts)
    norm = m + jnp.log(total)
    logp = (z_t - norm) * msk_ref[...].astype(jnp.float32)
    out_ref[0:1, :] = norm
    out_ref[1:2, :] = logp
    out_ref[2:3, :] = m - norm
    out_ref[3:4, :] = jnp.broadcast_to(jnp.sum(logp, axis=-1, keepdims=True), logp.shape)
    for c in copies:
        c.wait_send()


def solution(mesh):
    n_tp = mesh.shape["tp"]

    def local_part(hidden, ln_gain, ln_bias, embedding, targets, score_mask):
        _, tokens, width = hidden.shape
        rows = embedding.shape[0]
        n_chunks = width // CHUNK
        single = rows - 2 * SHARED
        vmem = pl.BlockSpec(memory_space=pltpu.VMEM)
        hbm = pl.BlockSpec(memory_space=pl.ANY)
        f32, bf16 = jnp.float32, jnp.bfloat16
        dma = pltpu.SemaphoreType.DMA
        n_group = 3 * n_tp - 1
        out = pl.pallas_call(
            functools.partial(kernel, n_tp),
            out_shape=jax.ShapeDtypeStruct((8, tokens), f32),
            in_specs=[hbm, vmem, vmem, hbm, vmem, vmem],
            out_specs=vmem,
            scratch_shapes=[
                pltpu.VMEM((tokens, width), bf16),
                pltpu.VMEM((n_chunks, 2 * tokens, CHUNK), bf16),
                pltpu.VMEM((n_chunks, tokens // 2, CHUNK), f32),
                pltpu.VMEM((n_chunks, tokens, CHUNK), f32),
                pltpu.VMEM((n_chunks, SHARED, CHUNK), bf16),
                pltpu.VMEM((SHARED, 2 * tokens), f32),
                pltpu.VMEM((single, tokens), f32),
                pltpu.VMEM((8, tokens), f32),
                pltpu.VMEM((2, 8, tokens), f32),
                pltpu.VMEM((8, tokens), f32),
                pltpu.VMEM((8, tokens), f32),
                pltpu.VMEM((n_tp - 1, 8, tokens), f32),
                pltpu.VMEM((n_tp, 8, tokens), f32),
                pltpu.VMEM((n_tp, 8, tokens), f32),
                dma, dma((n_chunks,)), dma((n_chunks,)), dma((n_chunks,)), dma((n_chunks,)), dma((n_chunks,)), dma((n_chunks,)),
                dma((2,)), dma((2,)), dma((n_group,)), dma((n_group,)),
            ],
            compiler_params=pltpu.CompilerParams(collective_id=0, has_side_effects=True, vmem_limit_bytes=67043328),
        )(hidden, ln_gain.reshape(1, width), ln_bias.reshape(1, width), embedding, targets, score_mask)
        return out[0:1], out[1:2], out[3, :1], out[2:3]

    row_spec = P("dp", None)
    return jax.shard_map(local_part, mesh=mesh, in_specs=(P("dp", None, None), P(), P(), P("tp", None), row_spec, row_spec), out_specs=(row_spec, row_spec, P("dp"), row_spec), check_vma=False)
```

```python
import functools

import jax
import jax.numpy as jnp
from jax import lax
from jax.experimental import pallas as pl
from jax.experimental.pallas import tpu as pltpu
from jax.sharding import PartitionSpec as P

OPT_VOCAB = 50272
LN_EPS = 1e-5
CHUNK = 512
SHARED = 5632
BLOCK = 704
MESH = pl.DeviceIdType.MESH
NEG_INF = float("-inf")
NT = (((1,), (1,)), ((), ()))


def kernel(n_tp, x_hbm, gain_hbm, bias_hbm, emb_hbm, tgt_hbm, msk_hbm, out_ref,
           gain_ref, bias_ref, tgt_ref, msk_ref, x_buf, h_buf, hs_buf, fr_buf, e_buf, z_buf, zs_buf, tg_send, tg_recv, own_send, far_send, own_recv, y_recv, z_recv,
           in_sem, x_sem, s_sem, e_sem, hs_sem, hr_sem, rs_sem, rr_sem, ts_sem, tr_sem, ss_sem, sr_sem):
    dp, tp = lax.axis_index("dp"), lax.axis_index("tp")
    rows, width = emb_hbm.shape
    tokens = x_buf.shape[0]
    half = tokens // 2
    n_slots = width // CHUNK
    last = n_slots
    short = CHUNK // 2
    single = rows - 2 * SHARED
    per_slot = SHARED // single
    first_single = n_slots - pl.cdiv(n_slots, per_slot)
    core, y, z = tp % 2, dp % 2, dp // 2
    parity = (y + z) % 2
    dp_y, dp_z = dp + 1 - 2 * y, dp + 2 - 4 * z
    dp_far = dp_y + core * (dp_z - dp_y)
    tp_other = tp + 1 - 2 * core
    first_row = tp * rows
    shared_row = pl.multiple_of(parity * SHARED, 16)
    mine = pl.ds(pl.multiple_of(core * half, half), half)

    def place(c):
        if isinstance(c, int) and c in (0, last):
            return 0, pl.ds(0 if c == 0 else short, short), pl.ds(0 if c == 0 else width - short, short)
        start = c * CHUNK - short
        return c, pl.ds(0, CHUNK), pl.ds(start if isinstance(c, int) else pl.multiple_of(start, short), CHUNK)

    def fetch_x():
        return pltpu.make_async_copy(x_hbm.at[0], x_buf, x_sem)

    def single_at(slot):
        return first_single + slot // per_slot, pl.ds(pl.multiple_of(slot % per_slot * single, 16), single)

    def fetch_single(c):
        slot, lanes, cols = place(c)
        at, sl = single_at(slot)
        return pltpu.make_async_copy(emb_hbm.at[pl.ds(2 * SHARED, single), cols], e_buf.at[at, sl, lanes], s_sem.at[c])

    def fetch_shared(c):
        slot, lanes, cols = place(c)
        return pltpu.make_async_copy(emb_hbm.at[pl.ds(shared_row, SHARED), cols], e_buf.at[slot, :, lanes], e_sem.at[c])

    def send_h(c):
        slot, lanes, _ = place(c)
        return pltpu.make_async_remote_copy(hs_buf.at[slot, :, lanes], fr_buf.at[slot, mine, lanes], hs_sem.at[c], hr_sem.at[c], device_id={"dp": dp_far, "tp": tp}, device_id_type=MESH)

    def relay_h(c):
        slot, lanes, _ = place(c)
        ref = fr_buf.at[slot, mine, lanes]
        return pltpu.make_async_remote_copy(ref, ref, rs_sem.at[c], rr_sem.at[c], device_id={"dp": dp, "tp": tp_other}, device_id_type=MESH)

    def send_targets(k):
        to = tp if k == 0 else tp_other
        return pltpu.make_async_remote_copy(tg_send, tg_recv.at[core], ts_sem.at[k], tr_sem.at[core], device_id={"dp": dp_far, "tp": to}, device_id_type=MESH)

    small = [pltpu.make_async_copy(src, dst, in_sem.at[i]) for i, (src, dst) in enumerate(
        [(tgt_hbm, tgt_ref), (gain_hbm, gain_ref), (bias_hbm, bias_ref), (msk_hbm, msk_ref)])]
    fetch_x().start()
    for c in small:
        c.start()
    for c in range(4):
        fetch_single(c).start()

    barrier = pltpu.get_barrier_semaphore()
    group = [(dp, k) for k in range(1, n_tp)] + [(dp_y, k) for k in range(n_tp)] + [(dp_z, k) for k in range(n_tp)]
    for d, k in group:
        pl.semaphore_signal(barrier, inc=1, device_id={"dp": d, "tp": (tp + k) % n_tp}, device_id_type=MESH)
    for c in small:
        c.wait()
    tg_send[...] = jnp.broadcast_to(tgt_ref[...].astype(jnp.float32), tg_send.shape)

    fetch_x().wait()
    for c in range(4, last + 1):
        fetch_single(c).start()

    def norm_rows(row):
        sl = pl.ds(pl.multiple_of(row, 16), 16)
        x = x_buf[sl, :].astype(jnp.float32)
        mean = jnp.mean(x, axis=-1, keepdims=True)
        c = x - mean
        var = jnp.mean(c * c, axis=-1, keepdims=True)
        h = (c * lax.rsqrt(var + LN_EPS) * gain_ref[...] + bias_ref[...]).astype(jnp.bfloat16)
        for k in range(last + 1):
            slot, lanes, cols = place(k)
            h_buf[slot, sl, lanes] = h[:, cols.start:cols.start + cols.size]
        return h

    def norm_sent(g, carry):
        h = norm_rows(core * half + g * 16).astype(jnp.float32)
        for k in range(last + 1):
            slot, lanes, cols = place(k)
            hs_buf[slot, pl.ds(pl.multiple_of(g * 16, 16), 16), lanes] = h[:, cols.start:cols.start + cols.size]
        return carry

    def norm_kept(g, carry):
        norm_rows((1 - core) * half + g * 16)
        return carry

    lax.fori_loop(0, half // 16, norm_sent, 0)
    fetch_shared(0).start()
    pl.semaphore_wait(barrier, len(group))
    for c in range(last + 1):
        send_h(c).start()
    for k in range(2):
        send_targets(k).start()
    lax.fori_loop(0, half // 16, norm_kept, 0)

    def single_dot(c):
        slot, lanes, _ = place(c)
        at, sl = single_at(slot)
        return lax.dot_general(e_buf[at, sl, lanes], h_buf[slot, 0:tokens, lanes], NT, preferred_element_type=jnp.float32)

    def single_chunk(c, carry):
        fetch_single(c).wait()

        @pl.when(c == 4)
        def _():
            fetch_shared(1).start()
        zs_buf[...] += single_dot(c)
        return carry

    fetch_single(0).wait()
    zs_buf[...] = single_dot(0)
    lax.fori_loop(1, last, single_chunk, 0)
    fetch_single(last).wait()
    zs_buf[...] += single_dot(last)

    sub = lax.broadcasted_iota(jnp.int32, (8, 1), 0)
    lane = lax.broadcasted_iota(jnp.int32, (1, tokens), 1)

    def online(z, start, target, state, limit=None):
        n_rows, lanes = z.shape
        z = z.reshape(n_rows // 8, 8, lanes)
        step = lax.broadcasted_iota(jnp.int32, z.shape, 0) * 8
        if limit is not None:
            z = jnp.where(step < (limit - start) - sub[None], z, NEG_INF)
        t8 = jnp.sum(jnp.where(step == (target - start - sub)[None], z, 0.0), axis=0)
        m8 = jnp.max(z, axis=0)
        if state is None:
            return m8, jnp.sum(jnp.exp(z - m8[None]), axis=0), t8
        m_new = jnp.maximum(state[0], m8)
        s8 = state[1] * jnp.exp(state[0] - m_new) + jnp.sum(jnp.exp(z - m_new[None]), axis=0)
        return m_new, s8, state[2] + t8

    def fold(state):
        m1 = jnp.max(state[0], axis=0, keepdims=True)
        return m1, jnp.sum(state[1] * jnp.exp(state[0] - m1), axis=0, keepdims=True), jnp.sum(state[2], axis=0, keepdims=True)

    send_h(0).wait_recv()
    relay_h(0).start()

    def shared_ready(c):
        fetch_shared(c).wait()
        if isinstance(c, int):
            if c + 1 <= last:
                send_h(c + 1).wait_recv()
                relay_h(c + 1).start()
            if c + 2 <= last:
                fetch_shared(c + 2).start()
        else:
            @pl.when(c + 1 < last)
            def _():
                send_h(c + 1).wait_recv()
                relay_h(c + 1).start()

            @pl.when(c + 1 == last)
            def _():
                send_h(last).wait_recv()
                relay_h(last).start()

            @pl.when(c + 2 < last)
            def _():
                fetch_shared(c + 2).start()

            @pl.when(c + 2 == last)
            def _():
                fetch_shared(last).start()
        relay_h(c).wait_recv()
        slot, lanes, _ = place(c)
        h_buf[slot, tokens:2 * tokens, lanes] = fr_buf[slot, :, lanes].astype(jnp.bfloat16)

    def shared_dot(c, sl):
        slot, lanes, _ = place(c)
        return lax.dot_general(e_buf[slot, sl, lanes], h_buf[slot, :, lanes], NT, preferred_element_type=jnp.float32)

    target = tgt_ref[...]
    every = pl.ds(0, SHARED)
    shared_ready(0)
    z_buf[...] = shared_dot(0, every)
    m_s, s_s, t_s = fold(online(zs_buf[...], first_row + 2 * SHARED, target, None, OPT_VOCAB))

    def shared_chunk(c, carry):
        shared_ready(c)
        z_buf[...] += shared_dot(c, every)
        return carry

    lax.fori_loop(1, last, shared_chunk, 0)

    for k in range(2):
        pltpu.make_async_remote_copy(tg_send, tg_recv.at[k], ts_sem.at[k], tr_sem.at[k], device_id={"dp": dp_far, "tp": tp}, device_id_type=MESH).wait_recv()
    far_target = jnp.where(lane < half, tg_recv[0, 0:1, :], tg_recv[1, 0:1, :]).astype(jnp.int32)
    both = jnp.concatenate([target, far_target], axis=1)
    shared_ready(last)

    def rows_of(i):
        return pl.ds(pl.multiple_of(i * BLOCK, BLOCK), BLOCK)

    def step(i, state):
        state = online(z_buf[rows_of(i), :], first_row + shared_row + i * BLOCK, both, state)

        if not isinstance(i, int):
            sl = rows_of(i + 1)
            z_buf[sl, :] += shared_dot(last, sl)
        return state

    z_buf[rows_of(0), :] += shared_dot(last, rows_of(0))
    n_blocks = SHARED // BLOCK
    empty = (jnp.full((8, 2 * tokens), NEG_INF), jnp.zeros((8, 2 * tokens), jnp.float32), jnp.zeros((8, 2 * tokens), jnp.float32))
    m_h, s_h, t_h = fold(step(n_blocks - 1, lax.fori_loop(0, n_blocks - 1, step, empty)))

    m_o = jnp.maximum(m_s, m_h[:, :tokens])
    s_o = s_s * jnp.exp(m_s - m_o) + s_h[:, :tokens] * jnp.exp(m_h[:, :tokens] - m_o)
    t_o = t_s + t_h[:, :tokens]
    own_send[0:1, :] = m_o
    own_send[1:2, :] = s_o
    own_send[2:3, :] = t_o
    far_send[0:1, :] = m_h[:, tokens:]
    far_send[1:2, :] = s_h[:, tokens:]
    far_send[2:3, :] = t_h[:, tokens:]

    copies = []
    for i, (d, k) in enumerate(group):
        src = own_send if i < n_tp - 1 else far_send
        dst = own_recv.at[k - 1] if i < n_tp - 1 else (y_recv.at[k] if i < 2 * n_tp - 1 else z_recv.at[k])
        copies.append(pltpu.make_async_remote_copy(src, dst, ss_sem.at[i], sr_sem.at[i], device_id={"dp": d, "tp": (tp + k) % n_tp}, device_id_type=MESH))
    for c in copies:
        c.start()
    for c in range(last + 1):
        send_h(c).wait_send()
        relay_h(c).wait_send()
    for k in range(2):
        send_targets(k).wait_send()
    for c in copies:
        c.wait_recv()

    parts = [(m_o, s_o, t_o)]
    for k in range(n_tp - 1):
        parts.append(tuple(own_recv[k, j:j + 1, :] for j in range(3)))
    for k in range(n_tp):
        parts.append(tuple(jnp.where(lane < half, y_recv[k, j:j + 1, :], z_recv[k, j:j + 1, :]) for j in range(3)))
    m = functools.reduce(jnp.maximum, [p[0] for p in parts])
    total = sum(p[1] * jnp.exp(p[0] - m) for p in parts)
    z_t = sum(p[2] for p in parts)
    norm = m + jnp.log(total)
    logp = (z_t - norm) * msk_ref[...].astype(jnp.float32)
    out_ref[0:1, :] = norm
    out_ref[1:2, :] = logp
    out_ref[2:3, :] = m - norm
    for c in copies:
        c.wait_send()


def finish(all_ref, norm_ref, logp_ref, seq_ref, top_ref):
    logp = all_ref[1:2, :]
    norm_ref[...] = all_ref[0:1, :]
    logp_ref[...] = logp
    top_ref[...] = all_ref[2:3, :]
    seq_ref[...] = jnp.sum(logp, axis=-1, keepdims=True)


def solution(mesh):
    n_tp = mesh.shape["tp"]

    def local_part(hidden, ln_gain, ln_bias, embedding, targets, score_mask):
        _, tokens, width = hidden.shape
        rows = embedding.shape[0]
        n_slots = width // CHUNK
        single = rows - 2 * SHARED
        vmem = pl.BlockSpec(memory_space=pltpu.VMEM)
        hbm = pl.BlockSpec(memory_space=pl.ANY)
        f32, bf16 = jnp.float32, jnp.bfloat16
        dma = pltpu.SemaphoreType.DMA
        n_group = 3 * n_tp - 1
        out = pl.pallas_call(
            functools.partial(kernel, n_tp),
            out_shape=jax.ShapeDtypeStruct((8, tokens), f32),
            in_specs=[hbm] * 6,
            out_specs=vmem,
            scratch_shapes=[
                pltpu.VMEM((1, width), f32),
                pltpu.VMEM((1, width), f32),
                pltpu.VMEM((1, tokens), jnp.int32),
                pltpu.VMEM((1, tokens), jnp.int32),
                pltpu.VMEM((tokens, width), bf16),
                pltpu.VMEM((n_slots, 2 * tokens, CHUNK), bf16),
                pltpu.VMEM((n_slots, tokens // 2, CHUNK), f32),
                pltpu.VMEM((n_slots, tokens, CHUNK), f32),
                pltpu.VMEM((n_slots, SHARED, CHUNK), bf16),
                pltpu.VMEM((SHARED, 2 * tokens), f32),
                pltpu.VMEM((single, tokens), f32),
                pltpu.VMEM((8, tokens), f32),
                pltpu.VMEM((2, 8, tokens), f32),
                pltpu.VMEM((8, tokens), f32),
                pltpu.VMEM((8, tokens), f32),
                pltpu.VMEM((n_tp - 1, 8, tokens), f32),
                pltpu.VMEM((n_tp, 8, tokens), f32),
                pltpu.VMEM((n_tp, 8, tokens), f32),
                dma((4,)), dma, *[dma((n_slots + 1,))] * 6,
                dma((2,)), dma((2,)), dma((n_group,)), dma((n_group,)),
            ],
            compiler_params=pltpu.CompilerParams(collective_id=0, has_side_effects=True, vmem_limit_bytes=67043328),
        )(hidden, ln_gain.reshape(1, width), ln_bias.reshape(1, width), embedding, targets, score_mask)
        row = jax.ShapeDtypeStruct((1, tokens), f32)
        norm, logp, seq, top = pl.pallas_call(
            finish, out_shape=(row, row, jax.ShapeDtypeStruct((1, 1), f32), row), in_specs=[vmem], out_specs=(vmem,) * 4,
        )(out)
        return norm, logp, seq.reshape(1), top

    row_spec = P("dp", None)
    return jax.shard_map(local_part, mesh=mesh, in_specs=(P("dp", None, None), P(), P(), P("tp", None), row_spec, row_spec), out_specs=(row_spec, row_spec, P("dp"), row_spec), check_vma=False)
```

```python
import functools

import jax
import jax.numpy as jnp
from jax import lax
from jax.experimental import pallas as pl
from jax.experimental.pallas import tpu as pltpu
from jax.sharding import PartitionSpec as P

OPT_VOCAB = 50272
LN_EPS = 1e-5
CHUNK = 512
SHARED = 5632
BLOCK = 704
MESH = pl.DeviceIdType.MESH
NEG_INF = float("-inf")
NT = (((1,), (1,)), ((), ()))


def kernel(n_tp, x_hbm, gain_hbm, bias_hbm, emb_hbm, tgt_hbm, msk_hbm, out_ref,
           gain_ref, bias_ref, tgt_ref, msk_ref, x_buf, h_buf, hs_buf, fr_buf, e_buf, z_buf, zs_buf, tg_send, tg_recv, own_send, far_send, own_recv, y_recv, z_recv,
           in_sem, x_sem, s_sem, e_sem, hs_sem, hr_sem, rs_sem, rr_sem, ts_sem, tr_sem, ss_sem, sr_sem):
    dp, tp = lax.axis_index("dp"), lax.axis_index("tp")
    rows, width = emb_hbm.shape
    tokens = x_buf.shape[0]
    half = tokens // 2
    n_slots = width // CHUNK
    last = n_slots
    short = CHUNK // 2
    single = rows - 2 * SHARED
    per_slot = SHARED // single
    first_single = n_slots - pl.cdiv(n_slots, per_slot)
    core, y, z = tp % 2, dp % 2, dp // 2
    parity = (y + z) % 2
    dp_y, dp_z = dp + 1 - 2 * y, dp + 2 - 4 * z
    dp_far = dp_y + core * (dp_z - dp_y)
    tp_other = tp + 1 - 2 * core
    first_row = tp * rows
    shared_row = pl.multiple_of(parity * SHARED, 16)
    mine = pl.ds(pl.multiple_of(core * half, half), half)

    def place(c):
        if isinstance(c, int) and c in (0, last):
            return 0, pl.ds(0 if c == 0 else short, short), pl.ds(0 if c == 0 else width - short, short)
        start = c * CHUNK - short
        return c, pl.ds(0, CHUNK), pl.ds(start if isinstance(c, int) else pl.multiple_of(start, short), CHUNK)

    def fetch_x():
        return pltpu.make_async_copy(x_hbm.at[0], x_buf, x_sem)

    def single_at(slot):
        return first_single + slot // per_slot, pl.ds(pl.multiple_of(slot % per_slot * single, 16), single)

    def fetch_single(c):
        slot, lanes, cols = place(c)
        at, sl = single_at(slot)
        return pltpu.make_async_copy(emb_hbm.at[pl.ds(2 * SHARED, single), cols], e_buf.at[at, sl, lanes], s_sem.at[c])

    def fetch_shared(c):
        slot, lanes, cols = place(c)
        return pltpu.make_async_copy(emb_hbm.at[pl.ds(shared_row, SHARED), cols], e_buf.at[slot, :, lanes], e_sem.at[c])

    def send_h(c):
        slot, lanes, _ = place(c)
        return pltpu.make_async_remote_copy(hs_buf.at[slot, :, lanes], fr_buf.at[slot, mine, lanes], hs_sem.at[c], hr_sem.at[c], device_id={"dp": dp_far, "tp": tp}, device_id_type=MESH)

    def relay_h(c):
        slot, lanes, _ = place(c)
        ref = fr_buf.at[slot, mine, lanes]
        return pltpu.make_async_remote_copy(ref, ref, rs_sem.at[c], rr_sem.at[c], device_id={"dp": dp, "tp": tp_other}, device_id_type=MESH)

    def send_targets(k):
        to = tp if k == 0 else tp_other
        return pltpu.make_async_remote_copy(tg_send, tg_recv.at[core], ts_sem.at[k], tr_sem.at[core], device_id={"dp": dp_far, "tp": to}, device_id_type=MESH)

    small = [pltpu.make_async_copy(src, dst, in_sem.at[i]) for i, (src, dst) in enumerate(
        [(tgt_hbm, tgt_ref), (gain_hbm, gain_ref), (bias_hbm, bias_ref), (msk_hbm, msk_ref)])]
    fetch_x().start()
    for c in small:
        c.start()
    for c in range(4):
        fetch_single(c).start(priority=1)

    barrier = pltpu.get_barrier_semaphore()
    group = [(dp, k) for k in range(1, n_tp)] + [(dp_y, k) for k in range(n_tp)] + [(dp_z, k) for k in range(n_tp)]
    for d, k in group:
        pl.semaphore_signal(barrier, inc=1, device_id={"dp": d, "tp": (tp + k) % n_tp}, device_id_type=MESH)
    for c in small:
        c.wait()
    tg_send[...] = jnp.broadcast_to(tgt_ref[...].astype(jnp.float32), tg_send.shape)

    fetch_x().wait()
    for c in range(4, last + 1):
        fetch_single(c).start(priority=1)

    def norm_rows(row):
        sl = pl.ds(pl.multiple_of(row, 16), 16)
        x = x_buf[sl, :].astype(jnp.float32)
        mean = jnp.mean(x, axis=-1, keepdims=True)
        c = x - mean
        var = jnp.mean(c * c, axis=-1, keepdims=True)
        h = (c * lax.rsqrt(var + LN_EPS) * gain_ref[...] + bias_ref[...]).astype(jnp.bfloat16)
        for k in range(last + 1):
            slot, lanes, cols = place(k)
            h_buf[slot, sl, lanes] = h[:, cols.start:cols.start + cols.size]
        return h

    def norm_sent(g, carry):
        h = norm_rows(core * half + g * 16).astype(jnp.float32)
        for k in range(last + 1):
            slot, lanes, cols = place(k)
            hs_buf[slot, pl.ds(pl.multiple_of(g * 16, 16), 16), lanes] = h[:, cols.start:cols.start + cols.size]
        return carry

    def norm_kept(g, carry):
        norm_rows((1 - core) * half + g * 16)
        return carry

    lax.fori_loop(0, half // 16, norm_sent, 0)
    fetch_shared(0).start(priority=1)
    pl.semaphore_wait(barrier, len(group))
    for c in range(last + 1):
        send_h(c).start()
    for k in range(2):
        send_targets(k).start()
    lax.fori_loop(0, half // 16, norm_kept, 0)

    def single_dot(c):
        slot, lanes, _ = place(c)
        at, sl = single_at(slot)
        return lax.dot_general(e_buf[at, sl, lanes], h_buf[slot, 0:tokens, lanes], NT, preferred_element_type=jnp.float32)

    def single_chunk(c, carry):
        fetch_single(c).wait()

        @pl.when(c == 4)
        def _():
            fetch_shared(1).start(priority=1)
        zs_buf[...] += single_dot(c)
        return carry

    fetch_single(0).wait()
    zs_buf[...] = single_dot(0)
    lax.fori_loop(1, last, single_chunk, 0)
    send_h(0).wait_recv()
    relay_h(0).start()
    fetch_single(last).wait()
    zs_buf[...] += single_dot(last)

    sub = lax.broadcasted_iota(jnp.int32, (8, 1), 0)
    lane = lax.broadcasted_iota(jnp.int32, (1, tokens), 1)

    def online(z, start, target, state, limit=None):
        n_rows, lanes = z.shape
        z = z.reshape(n_rows // 8, 8, lanes)
        step = lax.broadcasted_iota(jnp.int32, z.shape, 0) * 8
        if limit is not None:
            z = jnp.where(step < (limit - start) - sub[None], z, NEG_INF)
        t8 = jnp.sum(jnp.where(step == (target - start - sub)[None], z, 0.0), axis=0)
        m8 = jnp.max(z, axis=0)
        if state is None:
            return m8, jnp.sum(jnp.exp(z - m8[None]), axis=0), t8
        m_new = jnp.maximum(state[0], m8)
        s8 = state[1] * jnp.exp(state[0] - m_new) + jnp.sum(jnp.exp(z - m_new[None]), axis=0)
        return m_new, s8, state[2] + t8

    def fold(state):
        m1 = jnp.max(state[0], axis=0, keepdims=True)
        return m1, jnp.sum(state[1] * jnp.exp(state[0] - m1), axis=0, keepdims=True), jnp.sum(state[2], axis=0, keepdims=True)

    def shared_ready(c):
        fetch_shared(c).wait()
        if isinstance(c, int):
            if c + 1 <= last:
                send_h(c + 1).wait_recv()
                relay_h(c + 1).start()
            if c + 2 <= last:
                fetch_shared(c + 2).start(priority=1)
        else:
            @pl.when(c + 1 < last)
            def _():
                send_h(c + 1).wait_recv()
                relay_h(c + 1).start()

            @pl.when(c + 1 == last)
            def _():
                send_h(last).wait_recv()
                relay_h(last).start()

            @pl.when(c + 2 < last)
            def _():
                fetch_shared(c + 2).start(priority=1)

            @pl.when(c + 2 == last)
            def _():
                fetch_shared(last).start(priority=1)
        relay_h(c).wait_recv()
        slot, lanes, _ = place(c)
        h_buf[slot, tokens:2 * tokens, lanes] = fr_buf[slot, :, lanes].astype(jnp.bfloat16)

    def shared_dot(c, sl):
        slot, lanes, _ = place(c)
        return lax.dot_general(e_buf[slot, sl, lanes], h_buf[slot, :, lanes], NT, preferred_element_type=jnp.float32)

    target = tgt_ref[...]
    every = pl.ds(0, SHARED)
    shared_ready(0)
    z_buf[...] = shared_dot(0, every)
    m_s, s_s, t_s = fold(online(zs_buf[...], first_row + 2 * SHARED, target, None, OPT_VOCAB))

    def shared_chunk(c, carry):
        shared_ready(c)
        z_buf[...] += shared_dot(c, every)
        return carry

    lax.fori_loop(1, last, shared_chunk, 0)

    for k in range(2):
        pltpu.make_async_remote_copy(tg_send, tg_recv.at[k], ts_sem.at[k], tr_sem.at[k], device_id={"dp": dp_far, "tp": tp}, device_id_type=MESH).wait_recv()
    far_target = jnp.where(lane < half, tg_recv[0, 0:1, :], tg_recv[1, 0:1, :]).astype(jnp.int32)
    both = jnp.concatenate([target, far_target], axis=1)
    shared_ready(last)

    def rows_of(i):
        return pl.ds(pl.multiple_of(i * BLOCK, BLOCK), BLOCK)

    def step(i, state):
        state = online(z_buf[rows_of(i), :], first_row + shared_row + i * BLOCK, both, state)

        if not isinstance(i, int):
            sl = rows_of(i + 1)
            z_buf[sl, :] += shared_dot(last, sl)
        return state

    z_buf[rows_of(0), :] += shared_dot(last, rows_of(0))
    n_blocks = SHARED // BLOCK
    empty = (jnp.full((8, 2 * tokens), NEG_INF), jnp.zeros((8, 2 * tokens), jnp.float32), jnp.zeros((8, 2 * tokens), jnp.float32))
    m_h, s_h, t_h = fold(step(n_blocks - 1, lax.fori_loop(0, n_blocks - 1, step, empty)))

    m_o = jnp.maximum(m_s, m_h[:, :tokens])
    s_o = s_s * jnp.exp(m_s - m_o) + s_h[:, :tokens] * jnp.exp(m_h[:, :tokens] - m_o)
    t_o = t_s + t_h[:, :tokens]
    own_send[0:1, :] = m_o
    own_send[1:2, :] = s_o
    own_send[2:3, :] = t_o
    far_send[0:1, :] = m_h[:, tokens:]
    far_send[1:2, :] = s_h[:, tokens:]
    far_send[2:3, :] = t_h[:, tokens:]

    copies = []
    for i, (d, k) in enumerate(group):
        src = own_send if i < n_tp - 1 else far_send
        dst = own_recv.at[k - 1] if i < n_tp - 1 else (y_recv.at[k] if i < 2 * n_tp - 1 else z_recv.at[k])
        copies.append(pltpu.make_async_remote_copy(src, dst, ss_sem.at[i], sr_sem.at[i], device_id={"dp": d, "tp": (tp + k) % n_tp}, device_id_type=MESH))
    for c in copies:
        c.start()
    for c in range(last + 1):
        send_h(c).wait_send()
        relay_h(c).wait_send()
    for k in range(2):
        send_targets(k).wait_send()
    for c in copies:
        c.wait_recv()

    parts = [(m_o, s_o, t_o)]
    for k in range(n_tp - 1):
        parts.append(tuple(own_recv[k, j:j + 1, :] for j in range(3)))
    for k in range(n_tp):
        parts.append(tuple(jnp.where(lane < half, y_recv[k, j:j + 1, :], z_recv[k, j:j + 1, :]) for j in range(3)))
    m = functools.reduce(jnp.maximum, [p[0] for p in parts])
    total = sum(p[1] * jnp.exp(p[0] - m) for p in parts)
    z_t = sum(p[2] for p in parts)
    norm = m + jnp.log(total)
    logp = (z_t - norm) * msk_ref[...].astype(jnp.float32)
    out_ref[0:1, :] = norm
    out_ref[1:2, :] = logp
    out_ref[2:3, :] = m - norm
    for c in copies:
        c.wait_send()


def finish(all_ref, norm_ref, logp_ref, seq_ref, top_ref):
    logp = all_ref[1:2, :]
    norm_ref[...] = all_ref[0:1, :]
    logp_ref[...] = logp
    top_ref[...] = all_ref[2:3, :]
    seq_ref[...] = jnp.sum(logp, axis=-1, keepdims=True)


def solution(mesh):
    n_tp = mesh.shape["tp"]

    def local_part(hidden, ln_gain, ln_bias, embedding, targets, score_mask):
        _, tokens, width = hidden.shape
        rows = embedding.shape[0]
        n_slots = width // CHUNK
        single = rows - 2 * SHARED
        vmem = pl.BlockSpec(memory_space=pltpu.VMEM)
        hbm = pl.BlockSpec(memory_space=pl.ANY)
        f32, bf16 = jnp.float32, jnp.bfloat16
        dma = pltpu.SemaphoreType.DMA
        n_group = 3 * n_tp - 1
        out = pl.pallas_call(
            functools.partial(kernel, n_tp),
            out_shape=pltpu.VMEM((8, tokens), f32),
            in_specs=[hbm] * 6,
            out_specs=vmem,
            scratch_shapes=[
                pltpu.VMEM((1, width), f32),
                pltpu.VMEM((1, width), f32),
                pltpu.VMEM((1, tokens), jnp.int32),
                pltpu.VMEM((1, tokens), jnp.int32),
                pltpu.VMEM((tokens, width), bf16),
                pltpu.VMEM((n_slots, 2 * tokens, CHUNK), bf16),
                pltpu.VMEM((n_slots, tokens // 2, CHUNK), f32),
                pltpu.VMEM((n_slots, tokens, CHUNK), f32),
                pltpu.VMEM((n_slots, SHARED, CHUNK), bf16),
                pltpu.VMEM((SHARED, 2 * tokens), f32),
                pltpu.VMEM((single, tokens), f32),
                pltpu.VMEM((8, tokens), f32),
                pltpu.VMEM((2, 8, tokens), f32),
                pltpu.VMEM((8, tokens), f32),
                pltpu.VMEM((8, tokens), f32),
                pltpu.VMEM((n_tp - 1, 8, tokens), f32),
                pltpu.VMEM((n_tp, 8, tokens), f32),
                pltpu.VMEM((n_tp, 8, tokens), f32),
                dma((4,)), dma, *[dma((n_slots + 1,))] * 6,
                dma((2,)), dma((2,)), dma((n_group,)), dma((n_group,)),
            ],
            compiler_params=pltpu.CompilerParams(collective_id=0, has_side_effects=True, vmem_limit_bytes=63 << 20),
        )(hidden, ln_gain.reshape(1, width), ln_bias.reshape(1, width), embedding, targets, score_mask)
        row = jax.ShapeDtypeStruct((1, tokens), f32)
        norm, logp, seq, top = pl.pallas_call(
            finish, out_shape=(row, row, jax.ShapeDtypeStruct((1, 1), f32), row), in_specs=[vmem], out_specs=(vmem,) * 4,
        )(pltpu.with_memory_space_constraint(out, pltpu.VMEM))
        return norm, logp, seq.reshape(1), top

    row_spec = P("dp", None)
    return jax.shard_map(local_part, mesh=mesh, in_specs=(P("dp", None, None), P(), P(), P("tp", None), row_spec, row_spec), out_specs=(row_spec, row_spec, P("dp"), row_spec), check_vma=False)
```

```python
import functools

import jax
import jax.numpy as jnp
from jax import lax
from jax.experimental import pallas as pl
from jax.experimental.pallas import tpu as pltpu
from jax.sharding import PartitionSpec as P

OPT_VOCAB = 50272
LN_EPS = 1e-5
CHUNK = 512
SHARED = 5632
BLOCK = 352
HELD = 7
NORM_ROWS = 32
MESH = pl.DeviceIdType.MESH
NEG_INF = float("-inf")
NT = (((1,), (1,)), ((), ()))


def kernel(n_tp, x_hbm, gain_hbm, bias_hbm, emb_hbm, tgt_hbm, msk_hbm, out_ref,
           gain_ref, bias_ref, tgt_ref, msk_ref, x_buf, h_buf, hs_buf, fr_buf, e_buf, z_buf, zs_buf, tg_send, tg_recv, own_send, far_send, all_recv,
           in_sem, x_sem, s_sem, e_sem, hs_sem, hr_sem, rs_sem, rr_sem, ts_sem, tr_sem, ss_sem, sr_sem):
    dp, tp = lax.axis_index("dp"), lax.axis_index("tp")
    rows, width = emb_hbm.shape
    tokens = x_buf.shape[1]
    half = tokens // 2
    n_slots = width // CHUNK
    last = n_slots
    short = CHUNK // 2
    single = rows - 2 * SHARED
    per_slot = SHARED // single
    n_held = e_buf.shape[0]
    first_single = n_held - pl.cdiv(n_slots, per_slot)
    core, y, z = tp % 2, dp % 2, dp // 2
    parity = (y + z) % 2
    dp_y, dp_z = dp + 1 - 2 * y, dp + 2 - 4 * z
    dp_far = dp_y + core * (dp_z - dp_y)
    tp_other = tp + 1 - 2 * core
    first_row = tp * rows
    shared_row = pl.multiple_of(parity * SHARED, 16)
    mine = pl.ds(pl.multiple_of(core * half, half), half)
    rest = pl.ds(pl.multiple_of((1 - core) * half, half), half)

    def place(c):
        if isinstance(c, int) and c in (0, last):
            return 0, pl.ds(0 if c == 0 else short, short), pl.ds(0 if c == 0 else width - short, short)
        start = c * CHUNK - short
        return c, pl.ds(0, CHUNK), pl.ds(start if isinstance(c, int) else pl.multiple_of(start, short), CHUNK)

    def fetch_x(c, part, sl):
        slot, lanes, cols = place(c)
        return pltpu.make_async_copy(x_hbm.at[0, sl, cols], x_buf.at[slot, sl, lanes], x_sem.at[part])

    def wait_x(part, sl):
        ref = x_buf.at[:, sl]
        pltpu.make_async_copy(ref, ref, x_sem.at[part]).wait()

    def single_at(slot):
        return first_single + slot // per_slot, pl.ds(pl.multiple_of(slot % per_slot * single, 16), single)

    def fetch_single(c):
        slot, lanes, cols = place(c)
        at, sl = single_at(slot)
        return pltpu.make_async_copy(emb_hbm.at[pl.ds(2 * SHARED, single), cols], e_buf.at[at, sl, lanes], s_sem.at[slot])

    def wait_single(slot):
        at, sl = single_at(slot)
        ref = e_buf.at[at, sl]
        pltpu.make_async_copy(ref, ref, s_sem.at[slot]).wait()

    def held(c):
        return n_slots - n_held if isinstance(c, int) and n_held <= c < last else c

    def fetch_shared(c):
        slot, lanes, cols = place(c)
        return pltpu.make_async_copy(emb_hbm.at[pl.ds(shared_row, SHARED), cols], e_buf.at[held(slot), :, lanes], e_sem.at[c])

    def send_h(c):
        slot, lanes, _ = place(c)
        return pltpu.make_async_remote_copy(hs_buf.at[slot, :, lanes], fr_buf.at[slot, mine, lanes], hs_sem, hr_sem.at[c], device_id={"dp": dp_far, "tp": tp}, device_id_type=MESH)

    def relay_h(c):
        slot, lanes, _ = place(c)
        ref = fr_buf.at[slot, mine, lanes]
        return pltpu.make_async_remote_copy(ref, ref, rs_sem, rr_sem.at[c], device_id={"dp": dp, "tp": tp_other}, device_id_type=MESH)

    def send_targets(k):
        to = tp if k == 0 else tp_other
        return pltpu.make_async_remote_copy(tg_send, tg_recv.at[core], ts_sem, tr_sem, device_id={"dp": dp_far, "tp": to}, device_id_type=MESH)

    small = [pltpu.make_async_copy(src, dst, in_sem.at[i]) for i, (src, dst) in enumerate(
        [(tgt_hbm, tgt_ref), (gain_hbm, gain_ref), (bias_hbm, bias_ref), (msk_hbm, msk_ref)])]
    for part, sl in enumerate((mine, rest)):
        for c in range(last + 1):
            fetch_x(c, part, sl).start()
    for c in small:
        c.start()
    for c in (0, last, 1, 2, 3):
        fetch_single(c).start(priority=1)

    barrier = pltpu.get_barrier_semaphore()
    group = [(dp, k) for k in range(1, n_tp)] + [(dp_y, k) for k in range(n_tp)] + [(dp_z, k) for k in range(n_tp)]
    for d, k in group:
        pl.semaphore_signal(barrier, inc=1, device_id={"dp": d, "tp": (tp + k) % n_tp}, device_id_type=MESH)
    for c in small:
        c.wait()
    tg_send[...] = jnp.broadcast_to(tgt_ref[...].astype(jnp.float32), tg_send.shape)

    wait_x(0, mine)
    for c in range(4, last):
        fetch_single(c).start(priority=1)
    for c in range(2):
        fetch_shared(c).start(priority=1)

    def norm_rows(row):
        sl = pl.ds(pl.multiple_of(row, NORM_ROWS), NORM_ROWS)

        def load(k):
            return x_buf[k, sl, :].astype(jnp.float32)

        def cols(ref, k):
            if k == 0:
                return jnp.concatenate([ref[:, 0:short], ref[:, width - short:width]], axis=1)
            return ref[:, k * CHUNK - short:(k + 1) * CHUNK - short]

        mean = jnp.sum(sum(load(k) for k in range(n_slots)), axis=-1, keepdims=True) / width
        var = jnp.sum(sum((load(k) - mean) * (load(k) - mean) for k in range(n_slots)), axis=-1, keepdims=True) / width
        scale = lax.rsqrt(var + LN_EPS)
        for k in range(n_slots):
            h = ((load(k) - mean) * scale * cols(gain_ref, k) + cols(bias_ref, k)).astype(jnp.bfloat16)
            h_buf[k, sl, :] = h
            yield k, h

    def norm_sent(g, carry):
        for k, h in norm_rows(core * half + g * NORM_ROWS):
            hs_buf[k, pl.ds(pl.multiple_of(g * NORM_ROWS, NORM_ROWS), NORM_ROWS), :] = h.astype(jnp.float32)
        return carry

    def norm_kept(g, carry):
        for _ in norm_rows((1 - core) * half + g * NORM_ROWS):
            pass
        return carry

    lax.fori_loop(0, half // NORM_ROWS, norm_sent, 0)
    pl.semaphore_wait(barrier, len(group))
    for c in range(last + 1):
        send_h(c).start()
    for k in range(2):
        send_targets(k).start()
    wait_x(1, rest)
    lax.fori_loop(0, half // NORM_ROWS, norm_kept, 0)

    def single_dot(slot):
        at, sl = single_at(slot)
        return lax.dot_general(e_buf[at, sl, :], h_buf[slot, 0:tokens, :], NT, preferred_element_type=jnp.float32)

    zs_buf[...] = jnp.zeros_like(zs_buf)

    def single_step(i, carry):
        @pl.when(i == 2)
        def _():
            fetch_shared(2).start(priority=1)

        @pl.when(i == 3)
        def _():
            send_h(0).wait_recv()
            relay_h(0).start()
        for k in range(2):
            wait_single(2 * i + k)
        zs_buf[...] += single_dot(2 * i) + single_dot(2 * i + 1)
        return carry

    lax.fori_loop(0, n_slots // 2, single_step, 0)

    sub = lax.broadcasted_iota(jnp.int32, (8, 1), 0)
    lane = lax.broadcasted_iota(jnp.int32, (1, tokens), 1)

    def online(z, start, target, state, limit=None):
        n_rows, lanes = z.shape
        z = z.reshape(n_rows // 8, 8, lanes)
        step = lax.broadcasted_iota(jnp.int32, z.shape, 0) * 8
        if limit is not None:
            z = jnp.where(step < (limit - start) - sub[None], z, NEG_INF)
        t8 = jnp.sum(jnp.where(step == (target - start - sub)[None], z, 0.0), axis=0)
        m8 = jnp.max(z, axis=0)
        if state is None:
            return m8, jnp.sum(jnp.exp(z - m8[None]), axis=0), t8
        m_new = jnp.maximum(state[0], m8)
        s8 = state[1] * jnp.exp(state[0] - m_new) + jnp.sum(jnp.exp(z - m_new[None]), axis=0)
        return m_new, s8, state[2] + t8

    def fold(state):
        m1 = jnp.max(state[0], axis=0, keepdims=True)
        return m1, jnp.sum(state[1] * jnp.exp(state[0] - m1), axis=0, keepdims=True), jnp.sum(state[2], axis=0, keepdims=True)

    def shared_ready(c):
        fetch_shared(c).wait()
        if isinstance(c, int):
            if c + 2 <= last:
                send_h(c + 1).wait_recv()
                relay_h(c + 1).start()
            if c + 3 <= last:
                fetch_shared(c + 3).start(priority=1)
        else:
            @pl.when(c + 1 < last)
            def _():
                send_h(c + 1).wait_recv()
                relay_h(c + 1).start()

            @pl.when(c + 2 == last)
            def _():
                send_h(last).wait_recv()
                relay_h(last).start()

            @pl.when(c + 3 < n_held)
            def _():
                fetch_shared(c + 3).start(priority=1)

            for k in range(n_held, last + 1):
                @pl.when(c + 3 == k)
                def _():
                    fetch_shared(k).start(priority=1)
        relay_h(c).wait_recv()
        slot, lanes, _ = place(c)
        h_buf[slot, tokens:2 * tokens, lanes] = fr_buf[slot, :, lanes].astype(jnp.bfloat16)

    def shared_dot(c, sl):
        slot, lanes, _ = place(c)
        return lax.dot_general(e_buf[held(slot), sl, lanes], h_buf[slot, :, lanes], NT, preferred_element_type=jnp.float32)

    target = tgt_ref[...]
    every = pl.ds(0, SHARED)
    shared_ready(0)
    z_buf[...] = shared_dot(0, every)
    m_s, s_s, t_s = fold(online(zs_buf[...], first_row + 2 * SHARED, target, None, OPT_VOCAB))

    def shared_chunk(c, carry):
        shared_ready(c)
        z_buf[...] += shared_dot(c, every)
        return carry

    lax.fori_loop(1, last - 1, shared_chunk, 0)
    shared_ready(last - 1)
    shared_ready(last)
    z_buf[...] += shared_dot(last - 1, every) + shared_dot(last, every)

    pltpu.make_async_remote_copy(tg_recv, tg_recv, ts_sem, tr_sem, device_id={"dp": dp_far, "tp": tp}, device_id_type=MESH).wait_recv()
    far_target = jnp.where(lane < half, tg_recv[0, 0:1, :], tg_recv[1, 0:1, :]).astype(jnp.int32)
    both = jnp.concatenate([target, far_target], axis=1)
    n_blocks = SHARED // BLOCK

    def block(i):
        return z_buf[pl.ds(pl.multiple_of(i * BLOCK, BLOCK), BLOCK), :].reshape(BLOCK // 8, 8, 2 * tokens)

    def add(i, m8, s8, t8):
        zz = block(i)
        step = lax.broadcasted_iota(jnp.int32, zz.shape, 0) * 8
        t8 = t8 + jnp.sum(jnp.where(step == (both - (first_row + shared_row + i * BLOCK) - sub)[None], zz, 0.0), axis=0)
        return s8 + jnp.sum(jnp.exp(zz - m8[None]), axis=0), t8

    def step(i, state):
        m8, s8, t8 = state
        m_new = jnp.maximum(m8, jnp.max(block(i + 1), axis=0))
        s8, t8 = add(i, m8, s8, t8)
        return m_new, s8 * jnp.exp(m8 - m_new), t8

    zero = jnp.zeros((8, 2 * tokens), jnp.float32)
    m8, s8, t8 = lax.fori_loop(0, n_blocks - 1, step, (jnp.max(block(0), axis=0), zero, zero))
    m_h, s_h, t_h = fold((m8, *add(n_blocks - 1, m8, s8, t8)))

    m_o = jnp.maximum(m_s, m_h[:, :tokens])
    s_o = s_s * jnp.exp(m_s - m_o) + s_h[:, :tokens] * jnp.exp(m_h[:, :tokens] - m_o)
    t_o = t_s + t_h[:, :tokens]
    own_send[0:1, :] = m_o
    own_send[1:2, :] = s_o
    own_send[2:3, :] = t_o
    far_send[0:1, :] = m_h[:, tokens:]
    far_send[1:2, :] = s_h[:, tokens:]
    far_send[2:3, :] = t_h[:, tokens:]

    copies = []
    for i, (d, k) in enumerate(group):
        slot = k - 1 if i < n_tp - 1 else (n_tp - 1 + k if i < 2 * n_tp - 1 else 2 * n_tp - 1 + k)
        copies.append(pltpu.make_async_remote_copy(own_send if i < n_tp - 1 else far_send, all_recv.at[slot], ss_sem, sr_sem, device_id={"dp": d, "tp": (tp + k) % n_tp}, device_id_type=MESH))
    for c in copies[n_tp - 1:] + copies[:n_tp - 1]:
        c.start()

    def total_of(ref, send_sem, recv_sem):
        return pltpu.make_async_remote_copy(ref, ref, send_sem, recv_sem, device_id={"dp": dp, "tp": tp_other}, device_id_type=MESH)

    total_of(hs_buf, hs_sem, sr_sem).wait_send()
    total_of(hs_buf, rs_sem, sr_sem).wait_send()
    total_of(tg_recv, ts_sem, sr_sem).wait_send()
    total_of(all_recv, ss_sem, sr_sem).wait_recv()

    parts = [(m_o, s_o, t_o)]
    for k in range(n_tp - 1):
        parts.append(tuple(all_recv[k, j:j + 1, :] for j in range(3)))
    for k in range(n_tp - 1, 2 * n_tp - 1):
        parts.append(tuple(jnp.where(lane < half, all_recv[k, j:j + 1, :], all_recv[k + n_tp, j:j + 1, :]) for j in range(3)))
    m = functools.reduce(jnp.maximum, [p[0] for p in parts])
    total = sum(p[1] * jnp.exp(p[0] - m) for p in parts)
    z_t = sum(p[2] for p in parts)
    norm = m + jnp.log(total)
    logp = (z_t - norm) * msk_ref[...].astype(jnp.float32)
    out_ref[0:1, :] = norm
    out_ref[1:2, :] = logp
    out_ref[2:3, :] = m - norm
    total_of(all_recv, ss_sem, sr_sem).wait_send()


def finish(all_ref, norm_ref, logp_ref, seq_ref, top_ref):
    logp = all_ref[1:2, :]
    norm_ref[...] = all_ref[0:1, :]
    logp_ref[...] = logp
    top_ref[...] = all_ref[2:3, :]
    seq_ref[...] = jnp.sum(logp, axis=-1, keepdims=True)


def solution(mesh):
    n_tp = mesh.shape["tp"]

    def local_part(hidden, ln_gain, ln_bias, embedding, targets, score_mask):
        _, tokens, width = hidden.shape
        rows = embedding.shape[0]
        n_slots = width // CHUNK
        single = rows - 2 * SHARED
        vmem = pl.BlockSpec(memory_space=pltpu.VMEM)
        hbm = pl.BlockSpec(memory_space=pl.ANY)
        f32, bf16 = jnp.float32, jnp.bfloat16
        dma = pltpu.SemaphoreType.DMA
        n_group = 3 * n_tp - 1
        out = pl.pallas_call(
            functools.partial(kernel, n_tp),
            out_shape=pltpu.VMEM((8, tokens), f32),
            in_specs=[hbm] * 6,
            out_specs=vmem,
            scratch_shapes=[
                pltpu.VMEM((1, width), f32),
                pltpu.VMEM((1, width), f32),
                pltpu.VMEM((1, tokens), jnp.int32),
                pltpu.VMEM((1, tokens), jnp.int32),
                pltpu.VMEM((n_slots, tokens, CHUNK), bf16),
                pltpu.VMEM((n_slots, 2 * tokens, CHUNK), bf16),
                pltpu.VMEM((n_slots, tokens // 2, CHUNK), f32),
                pltpu.VMEM((n_slots, tokens, CHUNK), f32),
                pltpu.VMEM((HELD, SHARED, CHUNK), bf16),
                pltpu.VMEM((SHARED, 2 * tokens), f32),
                pltpu.VMEM((single, tokens), f32),
                pltpu.VMEM((8, tokens), f32),
                pltpu.VMEM((2, 8, tokens), f32),
                pltpu.VMEM((8, tokens), f32),
                pltpu.VMEM((8, tokens), f32),
                pltpu.VMEM((n_group, 8, tokens), f32),
                dma((4,)), dma((2,)), dma((n_slots,)), dma((n_slots + 1,)), dma, dma((n_slots + 1,)), dma, dma((n_slots + 1,)),
                dma, dma, dma, dma,
            ],
            compiler_params=pltpu.CompilerParams(collective_id=0, has_side_effects=True, vmem_limit_bytes=63 << 20),
        )(hidden, ln_gain.reshape(1, width), ln_bias.reshape(1, width), embedding, targets, score_mask)
        row = jax.ShapeDtypeStruct((1, tokens), f32)
        norm, logp, seq, top = pl.pallas_call(
            finish, out_shape=(row, row, jax.ShapeDtypeStruct((1, 1), f32), row), in_specs=[vmem], out_specs=(vmem,) * 4,
        )(pltpu.with_memory_space_constraint(out, pltpu.VMEM))
        return norm, logp, seq.reshape(1), top

    row_spec = P("dp", None)
    return jax.shard_map(local_part, mesh=mesh, in_specs=(P("dp", None, None), P(), P(), P("tp", None), row_spec, row_spec), out_specs=(row_spec, row_spec, P("dp"), row_spec), check_vma=False)
```

```python
import functools

import jax
import jax.numpy as jnp
from jax import lax
from jax.experimental import pallas as pl
from jax.experimental.pallas import tpu as pltpu
from jax.sharding import PartitionSpec as P

OPT_VOCAB = 50272
LN_EPS = 1e-5
CHUNK = 512
SHARED = 5632
BLOCK = 352
HELD = 7
NORM_ROWS = 32
MESH = pl.DeviceIdType.MESH
NEG_INF = float("-inf")
NT = (((1,), (1,)), ((), ()))


def kernel(n_tp, x_hbm, gain_hbm, bias_hbm, emb_hbm, tgt_hbm, msk_hbm, out_ref,
           gain_ref, bias_ref, tgt_ref, msk_ref, x_buf, h_buf, hs_buf, fr_buf, e_buf, z_buf, zs_buf, tg_send, tg_recv, own_send, far_send, all_recv,
           in_sem, x_sem, s_sem, e_sem, hs_sem, hr_sem, rs_sem, rr_sem, ts_sem, tr_sem, ss_sem, sr_sem):
    dp, tp = lax.axis_index("dp"), lax.axis_index("tp")
    rows, width = emb_hbm.shape
    tokens = x_buf.shape[1]
    half = tokens // 2
    n_slots = width // CHUNK
    last = n_slots
    short = CHUNK // 2
    single = rows - 2 * SHARED
    per_slot = SHARED // single
    n_held = e_buf.shape[0]
    first_single = n_held - pl.cdiv(n_slots, per_slot)
    core, y, z = tp % 2, dp % 2, dp // 2
    parity = (y + z) % 2
    dp_y, dp_z = dp + 1 - 2 * y, dp + 2 - 4 * z
    dp_far = dp_y + core * (dp_z - dp_y)
    tp_other = tp + 1 - 2 * core
    first_row = tp * rows
    shared_row = pl.multiple_of(parity * SHARED, 16)
    mine = pl.ds(pl.multiple_of(core * half, half), half)
    rest = pl.ds(pl.multiple_of((1 - core) * half, half), half)

    def place(c):
        if isinstance(c, int) and c in (0, last):
            return 0, pl.ds(0 if c == 0 else short, short), pl.ds(0 if c == 0 else width - short, short)
        start = c * CHUNK - short
        return c, pl.ds(0, CHUNK), pl.ds(start if isinstance(c, int) else pl.multiple_of(start, short), CHUNK)

    def fetch_x(c, part, sl):
        slot, lanes, cols = place(c)
        return pltpu.make_async_copy(x_hbm.at[0, sl, cols], x_buf.at[slot, sl, lanes], x_sem.at[part])

    def wait_x(part, sl):
        ref = x_buf.at[:, sl]
        pltpu.make_async_copy(ref, ref, x_sem.at[part]).wait()

    def single_at(slot):
        return first_single + slot // per_slot, pl.ds(pl.multiple_of(slot % per_slot * single, 16), single)

    def fetch_single(c):
        slot, lanes, cols = place(c)
        at, sl = single_at(slot)
        return pltpu.make_async_copy(emb_hbm.at[pl.ds(2 * SHARED, single), cols], e_buf.at[at, sl, lanes], s_sem.at[slot])

    def wait_single(slot):
        at, sl = single_at(slot)
        ref = e_buf.at[at, sl]
        pltpu.make_async_copy(ref, ref, s_sem.at[slot]).wait()

    def held(c):
        return n_slots - n_held if isinstance(c, int) and n_held <= c < last else c

    def fetch_shared(c):
        slot, lanes, cols = place(c)
        return pltpu.make_async_copy(emb_hbm.at[pl.ds(shared_row, SHARED), cols], e_buf.at[held(slot), :, lanes], e_sem.at[c])

    def send_h(c):
        slot, lanes, _ = place(c)
        return pltpu.make_async_remote_copy(hs_buf.at[slot, :, lanes], fr_buf.at[slot, mine, lanes], hs_sem, hr_sem.at[c], device_id={"dp": dp_far, "tp": tp}, device_id_type=MESH)

    def relay_h(c):
        slot, lanes, _ = place(c)
        ref = fr_buf.at[slot, mine, lanes]
        return pltpu.make_async_remote_copy(ref, ref, rs_sem, rr_sem.at[c], device_id={"dp": dp, "tp": tp_other}, device_id_type=MESH)

    def send_targets(k):
        to = tp if k == 0 else tp_other
        return pltpu.make_async_remote_copy(tg_send, tg_recv.at[core], ts_sem, tr_sem, device_id={"dp": dp_far, "tp": to}, device_id_type=MESH)

    small = [pltpu.make_async_copy(src, dst, in_sem.at[i]) for i, (src, dst) in enumerate(
        [(tgt_hbm, tgt_ref), (gain_hbm, gain_ref), (bias_hbm, bias_ref), (msk_hbm, msk_ref)])]
    for part, sl in enumerate((mine, rest)):
        for c in range(last + 1):
            fetch_x(c, part, sl).start()
    for c in small:
        c.start()
    for c in (0, last, 1, 2, 3):
        fetch_single(c).start(priority=1)

    barrier = pltpu.get_barrier_semaphore()
    group = [(dp, k) for k in range(1, n_tp)] + [(dp_y, k) for k in range(n_tp)] + [(dp_z, k) for k in range(n_tp)]
    for d, k in group:
        pl.semaphore_signal(barrier, inc=1, device_id={"dp": d, "tp": (tp + k) % n_tp}, device_id_type=MESH)
    for c in small:
        c.wait()
    tg_send[...] = jnp.broadcast_to(tgt_ref[...].astype(jnp.float32), tg_send.shape)

    wait_x(0, mine)
    for c in range(4, last):
        fetch_single(c).start(priority=1)
    for c in range(2):
        fetch_shared(c).start(priority=1)

    def norm_rows(row):
        sl = pl.ds(pl.multiple_of(row, NORM_ROWS), NORM_ROWS)

        def load(k):
            return x_buf[k, sl, :].astype(jnp.float32)

        def cols(ref, k):
            if k == 0:
                return jnp.concatenate([ref[:, 0:short], ref[:, width - short:width]], axis=1)
            return ref[:, k * CHUNK - short:(k + 1) * CHUNK - short]

        mean = jnp.sum(sum(load(k) for k in range(n_slots)), axis=-1, keepdims=True) / width
        var = jnp.sum(sum((load(k) - mean) * (load(k) - mean) for k in range(n_slots)), axis=-1, keepdims=True) / width
        scale = lax.rsqrt(var + LN_EPS)
        for k in range(n_slots):
            h = ((load(k) - mean) * scale * cols(gain_ref, k) + cols(bias_ref, k)).astype(jnp.bfloat16)
            h_buf[k, sl, :] = h
            yield k, h

    def norm_sent(g, carry):
        for k, h in norm_rows(core * half + g * NORM_ROWS):
            hs_buf[k, pl.ds(pl.multiple_of(g * NORM_ROWS, NORM_ROWS), NORM_ROWS), :] = h.astype(jnp.float32)
        return carry

    def norm_kept(g, carry):
        for _ in norm_rows((1 - core) * half + g * NORM_ROWS):
            pass
        return carry

    lax.fori_loop(0, half // NORM_ROWS, norm_sent, 0)
    pl.semaphore_wait(barrier, len(group))
    for c in range(last + 1):
        send_h(c).start()
    for k in range(2):
        send_targets(k).start()
    wait_x(1, rest)
    lax.fori_loop(0, half // NORM_ROWS, norm_kept, 0)

    def single_dot(slot):
        at, sl = single_at(slot)
        return lax.dot_general(e_buf[at, sl, :], h_buf[slot, 0:tokens, :], NT, preferred_element_type=jnp.float32)

    zs_buf[...] = jnp.zeros_like(zs_buf)

    def single_step(i, carry):
        @pl.when(i == 2)
        def _():
            fetch_shared(2).start(priority=1)

        @pl.when(i == 3)
        def _():
            send_h(0).wait_recv()
            relay_h(0).start()
        for k in range(2):
            wait_single(2 * i + k)
        zs_buf[...] += single_dot(2 * i) + single_dot(2 * i + 1)
        return carry

    lax.fori_loop(0, n_slots // 2, single_step, 0)

    sub = lax.broadcasted_iota(jnp.int32, (8, 1), 0)
    lane = lax.broadcasted_iota(jnp.int32, (1, tokens), 1)

    def online(z, start, target, state, limit=None):
        n_rows, lanes = z.shape
        z = z.reshape(n_rows // 8, 8, lanes)
        step = lax.broadcasted_iota(jnp.int32, z.shape, 0) * 8
        if limit is not None:
            z = jnp.where(step < (limit - start) - sub[None], z, NEG_INF)
        t8 = jnp.sum(jnp.where(step == (target - start - sub)[None], z, 0.0), axis=0)
        m8 = jnp.max(z, axis=0)
        if state is None:
            return m8, jnp.sum(jnp.exp(z - m8[None]), axis=0), t8
        m_new = jnp.maximum(state[0], m8)
        s8 = state[1] * jnp.exp(state[0] - m_new) + jnp.sum(jnp.exp(z - m_new[None]), axis=0)
        return m_new, s8, state[2] + t8

    def fold(state):
        m1 = jnp.max(state[0], axis=0, keepdims=True)
        return m1, jnp.sum(state[1] * jnp.exp(state[0] - m1), axis=0, keepdims=True), jnp.sum(state[2], axis=0, keepdims=True)

    def shared_ready(c):
        fetch_shared(c).wait()
        if isinstance(c, int):
            if c + 2 <= last:
                send_h(c + 1).wait_recv()
                relay_h(c + 1).start()
            if c + 3 <= last:
                fetch_shared(c + 3).start(priority=1)
        else:
            @pl.when(c + 1 < last)
            def _():
                send_h(c + 1).wait_recv()
                relay_h(c + 1).start()

            @pl.when(c + 2 == last)
            def _():
                send_h(last).wait_recv()
                relay_h(last).start()

            @pl.when(c + 3 < n_held)
            def _():
                fetch_shared(c + 3).start(priority=1)

            for k in range(n_held, last + 1):
                @pl.when(c + 3 == k)
                def _():
                    fetch_shared(k).start(priority=1)
        relay_h(c).wait_recv()
        slot, lanes, _ = place(c)
        h_buf[slot, tokens:2 * tokens, lanes] = fr_buf[slot, :, lanes].astype(jnp.bfloat16)

    def shared_dot(c, sl):
        slot, lanes, _ = place(c)
        return lax.dot_general(e_buf[held(slot), sl, lanes], h_buf[slot, :, lanes], NT, preferred_element_type=jnp.float32)

    target = tgt_ref[...]
    every = pl.ds(0, SHARED)
    shared_ready(0)
    z_buf[...] = shared_dot(0, every)
    m_s, s_s, t_s = fold(online(zs_buf[...], first_row + 2 * SHARED, target, None, OPT_VOCAB))

    def shared_chunk(c, carry):
        shared_ready(c)
        z_buf[...] += shared_dot(c, every)
        return carry

    lax.fori_loop(1, last - 1, shared_chunk, 0)
    shared_ready(last - 1)
    shared_ready(last)
    z_buf[...] += shared_dot(last - 1, every) + shared_dot(last, every)

    pltpu.make_async_remote_copy(tg_recv, tg_recv, ts_sem, tr_sem, device_id={"dp": dp_far, "tp": tp}, device_id_type=MESH).wait_recv()
    far_target = jnp.where(lane < half, tg_recv[0, 0:1, :], tg_recv[1, 0:1, :]).astype(jnp.int32)
    n_blocks = SHARED // BLOCK

    def shared_stats(first_lane, target):
        def block(i):
            return z_buf[pl.ds(pl.multiple_of(i * BLOCK, BLOCK), BLOCK), first_lane:first_lane + tokens].reshape(BLOCK // 8, 8, tokens)

        def add(i, m8, s8, t8):
            zz = block(i)
            step = lax.broadcasted_iota(jnp.int32, zz.shape, 0) * 8
            t8 = t8 + jnp.sum(jnp.where(step == (target - (first_row + shared_row + i * BLOCK) - sub)[None], zz, 0.0), axis=0)
            return s8 + jnp.sum(jnp.exp(zz - m8[None]), axis=0), t8

        def step(i, state):
            m8, s8, t8 = state
            m_new = jnp.maximum(m8, jnp.max(block(i + 1), axis=0))
            s8, t8 = add(i, m8, s8, t8)
            return m_new, s8 * jnp.exp(m8 - m_new), t8

        zero = jnp.zeros((8, tokens), jnp.float32)
        m8, s8, t8 = lax.fori_loop(0, n_blocks - 1, step, (jnp.max(block(0), axis=0), zero, zero))
        return fold((m8, *add(n_blocks - 1, m8, s8, t8)))

    def send_stats(src, first, end):
        for i, (d, k) in list(enumerate(group))[first:end]:
            slot = k - 1 if i < n_tp - 1 else (n_tp - 1 + k if i < 2 * n_tp - 1 else 2 * n_tp - 1 + k)
            pltpu.make_async_remote_copy(src, all_recv.at[slot], ss_sem, sr_sem, device_id={"dp": d, "tp": (tp + k) % n_tp}, device_id_type=MESH).start()

    for j, v in enumerate(shared_stats(tokens, far_target)):
        far_send[j:j + 1, :] = v
    send_stats(far_send, n_tp - 1, len(group))
    m_h, s_h, t_h = shared_stats(0, target)
    m_o = jnp.maximum(m_s, m_h)
    s_o = s_s * jnp.exp(m_s - m_o) + s_h * jnp.exp(m_h - m_o)
    t_o = t_s + t_h
    for j, v in enumerate((m_o, s_o, t_o)):
        own_send[j:j + 1, :] = v
    send_stats(own_send, 0, n_tp - 1)

    def total_of(ref, send_sem, recv_sem):
        return pltpu.make_async_remote_copy(ref, ref, send_sem, recv_sem, device_id={"dp": dp, "tp": tp_other}, device_id_type=MESH)

    total_of(hs_buf, hs_sem, sr_sem).wait_send()
    total_of(hs_buf, rs_sem, sr_sem).wait_send()
    total_of(tg_recv, ts_sem, sr_sem).wait_send()
    total_of(all_recv, ss_sem, sr_sem).wait_recv()

    parts = [(m_o, s_o, t_o)]
    for k in range(n_tp - 1):
        parts.append(tuple(all_recv[k, j:j + 1, :] for j in range(3)))
    for k in range(n_tp - 1, 2 * n_tp - 1):
        parts.append(tuple(jnp.where(lane < half, all_recv[k, j:j + 1, :], all_recv[k + n_tp, j:j + 1, :]) for j in range(3)))
    m = functools.reduce(jnp.maximum, [p[0] for p in parts])
    total = sum(p[1] * jnp.exp(p[0] - m) for p in parts)
    z_t = sum(p[2] for p in parts)
    norm = m + jnp.log(total)
    logp = (z_t - norm) * msk_ref[...].astype(jnp.float32)
    out_ref[0:1, :] = norm
    out_ref[1:2, :] = logp
    out_ref[2:3, :] = m - norm
    total_of(all_recv, ss_sem, sr_sem).wait_send()


def finish(all_ref, norm_ref, logp_ref, seq_ref, top_ref):
    logp = all_ref[1:2, :]
    norm_ref[...] = all_ref[0:1, :]
    logp_ref[...] = logp
    top_ref[...] = all_ref[2:3, :]
    seq_ref[...] = jnp.sum(logp, axis=-1, keepdims=True)


def solution(mesh):
    n_tp = mesh.shape["tp"]

    def local_part(hidden, ln_gain, ln_bias, embedding, targets, score_mask):
        _, tokens, width = hidden.shape
        rows = embedding.shape[0]
        n_slots = width // CHUNK
        single = rows - 2 * SHARED
        vmem = pl.BlockSpec(memory_space=pltpu.VMEM)
        hbm = pl.BlockSpec(memory_space=pl.ANY)
        f32, bf16 = jnp.float32, jnp.bfloat16
        dma = pltpu.SemaphoreType.DMA
        n_group = 3 * n_tp - 1
        out = pl.pallas_call(
            functools.partial(kernel, n_tp),
            out_shape=pltpu.VMEM((8, tokens), f32),
            in_specs=[hbm] * 6,
            out_specs=vmem,
            scratch_shapes=[
                pltpu.VMEM((1, width), f32),
                pltpu.VMEM((1, width), f32),
                pltpu.VMEM((1, tokens), jnp.int32),
                pltpu.VMEM((1, tokens), jnp.int32),
                pltpu.VMEM((n_slots, tokens, CHUNK), bf16),
                pltpu.VMEM((n_slots, 2 * tokens, CHUNK), bf16),
                pltpu.VMEM((n_slots, tokens // 2, CHUNK), f32),
                pltpu.VMEM((n_slots, tokens, CHUNK), f32),
                pltpu.VMEM((HELD, SHARED, CHUNK), bf16),
                pltpu.VMEM((SHARED, 2 * tokens), f32),
                pltpu.VMEM((single, tokens), f32),
                pltpu.VMEM((8, tokens), f32),
                pltpu.VMEM((2, 8, tokens), f32),
                pltpu.VMEM((8, tokens), f32),
                pltpu.VMEM((8, tokens), f32),
                pltpu.VMEM((n_group, 8, tokens), f32),
                dma((4,)), dma((2,)), dma((n_slots,)), dma((n_slots + 1,)), dma, dma((n_slots + 1,)), dma, dma((n_slots + 1,)),
                dma, dma, dma, dma,
            ],
            compiler_params=pltpu.CompilerParams(collective_id=0, has_side_effects=True, vmem_limit_bytes=63 << 20),
        )(hidden, ln_gain.reshape(1, width), ln_bias.reshape(1, width), embedding, targets, score_mask)
        row = jax.ShapeDtypeStruct((1, tokens), f32)
        norm, logp, seq, top = pl.pallas_call(
            finish, out_shape=(row, row, jax.ShapeDtypeStruct((1, 1), f32), row), in_specs=[vmem], out_specs=(vmem,) * 4,
        )(pltpu.with_memory_space_constraint(out, pltpu.VMEM))
        return norm, logp, seq.reshape(1), top

    row_spec = P("dp", None)
    return jax.shard_map(local_part, mesh=mesh, in_specs=(P("dp", None, None), P(), P(), P("tp", None), row_spec, row_spec), out_specs=(row_spec, row_spec, P("dp"), row_spec), check_vma=False)
```

```python
import functools

import jax
import jax.numpy as jnp
from jax import lax
from jax.experimental import pallas as pl
from jax.experimental.pallas import tpu as pltpu
from jax.sharding import PartitionSpec as P

OPT_VOCAB = 50272
LN_EPS = 1e-5
CHUNK = 512
SHARED = 5632
BLOCK = 256
HELD = 7
NORM_ROWS = 64
MESH = pl.DeviceIdType.MESH
NEG_INF = float("-inf")
NT = (((1,), (1,)), ((), ()))


def kernel(n_tp, x_hbm, gain_hbm, bias_hbm, emb_hbm, tgt_hbm, msk_hbm, out_ref,
           gain_ref, bias_ref, tgt_ref, msk_ref, x_buf, h_buf, hs_buf, fr_buf, e_buf, z_buf, zs_buf, tg_send, tg_recv, own_send, far_send, all_recv,
           in_sem, x_sem, s_sem, e_sem, hs_sem, hr_sem, rs_sem, rr_sem, ts_sem, tr_sem, ss_sem, sr_sem):
    dp, tp = lax.axis_index("dp"), lax.axis_index("tp")
    rows, width = emb_hbm.shape
    tokens = x_buf.shape[1]
    half = tokens // 2
    n_slots = width // CHUNK
    last = n_slots
    short = CHUNK // 2
    single = rows - 2 * SHARED
    per_slot = SHARED // single
    n_held = e_buf.shape[0]
    first_single = n_held - pl.cdiv(n_slots, per_slot)
    core, y, z = tp % 2, dp % 2, dp // 2
    parity = (y + z) % 2
    dp_y, dp_z = dp + 1 - 2 * y, dp + 2 - 4 * z
    dp_far = dp_y + core * (dp_z - dp_y)
    tp_other = tp + 1 - 2 * core
    first_row = tp * rows
    shared_row = pl.multiple_of(parity * SHARED, 16)
    mine = pl.ds(pl.multiple_of(core * half, half), half)
    rest = pl.ds(pl.multiple_of((1 - core) * half, half), half)

    def place(c, halves=False):
        if halves or (isinstance(c, int) and c < 2):
            lanes = pl.ds(c * short if isinstance(c, int) else pl.multiple_of(c * short, short), short)
            return 0, lanes, lanes
        start = (c - 1) * CHUNK
        return c - 1, pl.ds(0, CHUNK), pl.ds(start if isinstance(c, int) else pl.multiple_of(start, CHUNK), CHUNK)

    def fetch_x(c, part, sl):
        slot, lanes, cols = place(c)
        return pltpu.make_async_copy(x_hbm.at[0, sl, cols], x_buf.at[slot, sl, lanes], x_sem.at[part])

    def wait_x(part, sl):
        ref = x_buf.at[:, sl]
        pltpu.make_async_copy(ref, ref, x_sem.at[part]).wait()

    def single_at(slot):
        return first_single + slot // per_slot, pl.ds(pl.multiple_of(slot % per_slot * single, 16), single)

    def fetch_single(c):
        slot, lanes, cols = place(c)
        at, sl = single_at(slot)
        return pltpu.make_async_copy(emb_hbm.at[pl.ds(2 * SHARED, single), cols], e_buf.at[at, sl, lanes], s_sem.at[slot])

    def wait_single(slot):
        at, sl = single_at(slot)
        ref = e_buf.at[at, sl]
        pltpu.make_async_copy(ref, ref, s_sem.at[slot]).wait()

    def held(c):
        return n_slots - n_held if isinstance(c, int) and n_held <= c < last else c

    def fetch_shared(c, halves=False):
        slot, lanes, cols = place(c, halves)
        return pltpu.make_async_copy(emb_hbm.at[pl.ds(shared_row, SHARED), cols], e_buf.at[held(slot), :, lanes], e_sem.at[c])

    def send_h(c):
        slot, lanes, _ = place(c)
        return pltpu.make_async_remote_copy(hs_buf.at[slot, :, lanes], fr_buf.at[slot, mine, lanes], hs_sem, hr_sem.at[c], device_id={"dp": dp_far, "tp": tp}, device_id_type=MESH)

    def relay_h(c, halves=False):
        slot, lanes, _ = place(c, halves)
        ref = fr_buf.at[slot, mine, lanes]
        return pltpu.make_async_remote_copy(ref, ref, rs_sem, rr_sem.at[c], device_id={"dp": dp, "tp": tp_other}, device_id_type=MESH)

    def send_targets(k):
        to = tp if k == 0 else tp_other
        return pltpu.make_async_remote_copy(tg_send, tg_recv.at[core], ts_sem, tr_sem, device_id={"dp": dp_far, "tp": to}, device_id_type=MESH)

    small = [pltpu.make_async_copy(src, dst, in_sem.at[i]) for i, (src, dst) in enumerate(
        [(tgt_hbm, tgt_ref), (gain_hbm, gain_ref), (bias_hbm, bias_ref), (msk_hbm, msk_ref)])]
    for part, sl in enumerate((mine, rest)):
        for c in range(last + 1):
            fetch_x(c, part, sl).start()
    for c in small:
        c.start()
    for c in range(5):
        fetch_single(c).start(priority=1)

    barrier = pltpu.get_barrier_semaphore()
    group = [(dp, k) for k in range(1, n_tp)] + [(dp_y, k) for k in range(n_tp)] + [(dp_z, k) for k in range(n_tp)]
    for d, k in group:
        pl.semaphore_signal(barrier, inc=1, device_id={"dp": d, "tp": (tp + k) % n_tp}, device_id_type=MESH)
    for c in small:
        c.wait()
    tg_send[...] = jnp.broadcast_to(tgt_ref[...].astype(jnp.float32), tg_send.shape)

    wait_x(0, mine)
    for c in range(5, last + 1):
        fetch_single(c).start(priority=1)
    for c in range(3):
        fetch_shared(c).start(priority=1)

    def norm_rows(row):
        sl = pl.ds(pl.multiple_of(row, NORM_ROWS), NORM_ROWS)

        def load(k):
            return x_buf[k, sl, :].astype(jnp.float32)

        def cols(ref, k):
            return ref[:, k * CHUNK:(k + 1) * CHUNK]

        mean = jnp.sum(sum(load(k) for k in range(n_slots)), axis=-1, keepdims=True) / width
        var = jnp.sum(sum((load(k) - mean) * (load(k) - mean) for k in range(n_slots)), axis=-1, keepdims=True) / width
        scale = lax.rsqrt(var + LN_EPS)
        for k in range(n_slots):
            h = ((load(k) - mean) * scale * cols(gain_ref, k) + cols(bias_ref, k)).astype(jnp.bfloat16)
            h_buf[k, sl, :] = h
            yield k, h

    def norm_sent(g, carry):
        for k, h in norm_rows(core * half + g * NORM_ROWS):
            hs_buf[k, pl.ds(pl.multiple_of(g * NORM_ROWS, NORM_ROWS), NORM_ROWS), :] = h.astype(jnp.float32)
        return carry

    def norm_kept(g, carry):
        for _ in norm_rows((1 - core) * half + g * NORM_ROWS):
            pass
        return carry

    lax.fori_loop(0, half // NORM_ROWS, norm_sent, 0)
    pl.semaphore_wait(barrier, len(group))
    for c in range(last + 1):
        send_h(c).start()
    for k in range(2):
        send_targets(k).start()
    wait_x(1, rest)
    lax.fori_loop(0, half // NORM_ROWS, norm_kept, 0)

    def single_dot(slot):
        at, sl = single_at(slot)
        return lax.dot_general(e_buf[at, sl, :], h_buf[slot, 0:tokens, :], NT, preferred_element_type=jnp.float32)

    zs_buf[...] = jnp.zeros_like(zs_buf)

    def single_step(i, carry):
        @pl.when(i == 2)
        def _():
            fetch_shared(3).start(priority=1)

        @pl.when(i == 3)
        def _():
            send_h(0).wait_recv()
            relay_h(0).start()
        for k in range(2):
            wait_single(2 * i + k)
        zs_buf[...] += single_dot(2 * i) + single_dot(2 * i + 1)
        return carry

    lax.fori_loop(0, n_slots // 2, single_step, 0)

    sub = lax.broadcasted_iota(jnp.int32, (8, 1), 0)
    lane = lax.broadcasted_iota(jnp.int32, (1, tokens), 1)

    def online(z, start, target, state, limit=None):
        n_rows, lanes = z.shape
        z = z.reshape(n_rows // 8, 8, lanes)
        step = lax.broadcasted_iota(jnp.int32, z.shape, 0) * 8
        if limit is not None:
            z = jnp.where(step < (limit - start) - sub[None], z, NEG_INF)
        t8 = jnp.sum(jnp.where(step == (target - start - sub)[None], z, 0.0), axis=0)
        m8 = jnp.max(z, axis=0)
        if state is None:
            return m8, jnp.sum(jnp.exp(z - m8[None]), axis=0), t8
        m_new = jnp.maximum(state[0], m8)
        s8 = state[1] * jnp.exp(state[0] - m_new) + jnp.sum(jnp.exp(z - m_new[None]), axis=0)
        return m_new, s8, state[2] + t8

    def fold(state):
        m1 = jnp.max(state[0], axis=0, keepdims=True)
        return m1, jnp.sum(state[1] * jnp.exp(state[0] - m1), axis=0, keepdims=True), jnp.sum(state[2], axis=0, keepdims=True)

    def pass_on(c):
        send_h(c).wait_recv()
        relay_h(c).start()

    def shared_ready(c, halves=False):
        fetch_shared(c, halves).wait()
        if isinstance(c, int):
            if c + 1 <= last:
                pass_on(c + 1)
            if c + 4 <= last:
                fetch_shared(c + 4).start(priority=1)
        elif halves:
            pass_on(2)
            fetch_shared(5).start(priority=1)
        else:
            pass_on(c + 1)

            @pl.when(c + 4 < n_held)
            def _():
                fetch_shared(c + 4).start(priority=1)

            for k in range(n_held, last + 1):
                @pl.when(c + 4 == k)
                def _():
                    fetch_shared(k).start(priority=1)
        relay_h(c, halves).wait_recv()
        slot, lanes, _ = place(c, halves)
        h_buf[slot, tokens:2 * tokens, lanes] = fr_buf[slot, :, lanes].astype(jnp.bfloat16)

    def shared_dot(c, sl, halves=False):
        slot, lanes, _ = place(c, halves)
        return lax.dot_general(e_buf[held(slot), sl, lanes], h_buf[slot, :, lanes], NT, preferred_element_type=jnp.float32)

    target = tgt_ref[...]
    every = pl.ds(0, SHARED)
    shared_ready(0)
    z_buf[...] = shared_dot(0, every)
    m_s, s_s, t_s = fold(online(zs_buf[...], first_row + 2 * SHARED, target, None, OPT_VOCAB))

    def shared_chunk(c, carry):
        shared_ready(c)
        z_buf[...] += shared_dot(c, every)
        return carry

    def second_half(c, carry):
        shared_ready(c, True)
        z_buf[...] += shared_dot(c, every, True)
        return carry

    lax.fori_loop(1, 2 + dp // 1024, second_half, 0)
    lax.fori_loop(2, last, shared_chunk, 0)
    shared_ready(last)
    z_buf[...] += shared_dot(last, every)

    pltpu.make_async_remote_copy(tg_recv, tg_recv, ts_sem, tr_sem, device_id={"dp": dp_far, "tp": tp}, device_id_type=MESH).wait_recv()
    far_target = jnp.where(lane < half, tg_recv[0, 0:1, :], tg_recv[1, 0:1, :]).astype(jnp.int32)
    n_blocks = SHARED // BLOCK

    def shared_stats(first_lane, target):
        def block(i):
            return z_buf[pl.ds(pl.multiple_of(i * BLOCK, BLOCK), BLOCK), first_lane:first_lane + tokens].reshape(BLOCK // 8, 8, tokens)

        def add(i, m8, s8, t8):
            zz = block(i)
            step = lax.broadcasted_iota(jnp.int32, zz.shape, 0) * 8
            t8 = t8 + jnp.sum(jnp.where(step == (target - (first_row + shared_row + i * BLOCK) - sub)[None], zz, 0.0), axis=0)
            return s8 + jnp.sum(jnp.exp(zz - m8[None]), axis=0), t8

        def step(i, state):
            m8, s8, t8 = state
            m_new = jnp.maximum(m8, jnp.max(block(i + 1), axis=0))
            s8, t8 = add(i, m8, s8, t8)
            return m_new, s8 * jnp.exp(m8 - m_new), t8

        zero = jnp.zeros((8, tokens), jnp.float32)
        m8, s8, t8 = lax.fori_loop(0, n_blocks - 1, step, (jnp.max(block(0), axis=0), zero, zero))
        return fold((m8, *add(n_blocks - 1, m8, s8, t8)))

    def send_stats(src, first, end):
        for i, (d, k) in list(enumerate(group))[first:end]:
            slot = k - 1 if i < n_tp - 1 else (n_tp - 1 + k if i < 2 * n_tp - 1 else 2 * n_tp - 1 + k)
            pltpu.make_async_remote_copy(src, all_recv.at[slot], ss_sem, sr_sem, device_id={"dp": d, "tp": (tp + k) % n_tp}, device_id_type=MESH).start()

    for j, v in enumerate(shared_stats(tokens, far_target)):
        far_send[j:j + 1, :] = v
    send_stats(far_send, n_tp - 1, len(group))
    m_h, s_h, t_h = shared_stats(0, target)
    m_o = jnp.maximum(m_s, m_h)
    s_o = s_s * jnp.exp(m_s - m_o) + s_h * jnp.exp(m_h - m_o)
    t_o = t_s + t_h
    for j, v in enumerate((m_o, s_o, t_o)):
        own_send[j:j + 1, :] = v
    send_stats(own_send, 0, n_tp - 1)

    def total_of(ref, send_sem, recv_sem):
        return pltpu.make_async_remote_copy(ref, ref, send_sem, recv_sem, device_id={"dp": dp, "tp": tp_other}, device_id_type=MESH)

    total_of(hs_buf, hs_sem, sr_sem).wait_send()
    total_of(hs_buf, rs_sem, sr_sem).wait_send()
    total_of(tg_recv, ts_sem, sr_sem).wait_send()
    total_of(all_recv, ss_sem, sr_sem).wait_recv()

    parts = [(m_o, s_o, t_o)]
    for k in range(n_tp - 1):
        parts.append(tuple(all_recv[k, j:j + 1, :] for j in range(3)))
    for k in range(n_tp - 1, 2 * n_tp - 1):
        parts.append(tuple(jnp.where(lane < half, all_recv[k, j:j + 1, :], all_recv[k + n_tp, j:j + 1, :]) for j in range(3)))
    m = functools.reduce(jnp.maximum, [p[0] for p in parts])
    total = sum(p[1] * jnp.exp(p[0] - m) for p in parts)
    z_t = sum(p[2] for p in parts)
    norm = m + jnp.log(total)
    logp = (z_t - norm) * msk_ref[...].astype(jnp.float32)
    out_ref[0:1, :] = norm
    out_ref[1:2, :] = logp
    out_ref[2:3, :] = m - norm
    total_of(all_recv, ss_sem, sr_sem).wait_send()


def finish(all_ref, norm_ref, logp_ref, seq_ref, top_ref):
    logp = all_ref[1:2, :]
    norm_ref[...] = all_ref[0:1, :]
    logp_ref[...] = logp
    top_ref[...] = all_ref[2:3, :]
    seq_ref[...] = jnp.sum(logp, axis=-1, keepdims=True)


def solution(mesh):
    n_tp = mesh.shape["tp"]

    def local_part(hidden, ln_gain, ln_bias, embedding, targets, score_mask):
        _, tokens, width = hidden.shape
        rows = embedding.shape[0]
        n_slots = width // CHUNK
        single = rows - 2 * SHARED
        vmem = pl.BlockSpec(memory_space=pltpu.VMEM)
        hbm = pl.BlockSpec(memory_space=pl.ANY)
        f32, bf16 = jnp.float32, jnp.bfloat16
        dma = pltpu.SemaphoreType.DMA
        n_group = 3 * n_tp - 1
        out = pl.pallas_call(
            functools.partial(kernel, n_tp),
            out_shape=pltpu.VMEM((8, tokens), f32),
            in_specs=[hbm] * 6,
            out_specs=vmem,
            scratch_shapes=[
                pltpu.VMEM((1, width), f32),
                pltpu.VMEM((1, width), f32),
                pltpu.VMEM((1, tokens), jnp.int32),
                pltpu.VMEM((1, tokens), jnp.int32),
                pltpu.VMEM((n_slots, tokens, CHUNK), bf16),
                pltpu.VMEM((n_slots, 2 * tokens, CHUNK), bf16),
                pltpu.VMEM((n_slots, tokens // 2, CHUNK), f32),
                pltpu.VMEM((n_slots, tokens, CHUNK), f32),
                pltpu.VMEM((HELD, SHARED, CHUNK), bf16),
                pltpu.VMEM((SHARED, 2 * tokens), f32),
                pltpu.VMEM((single, tokens), f32),
                pltpu.VMEM((8, tokens), f32),
                pltpu.VMEM((2, 8, tokens), f32),
                pltpu.VMEM((8, tokens), f32),
                pltpu.VMEM((8, tokens), f32),
                pltpu.VMEM((n_group, 8, tokens), f32),
                dma((4,)), dma((2,)), dma((n_slots,)), dma((n_slots + 1,)), dma, dma((n_slots + 1,)), dma, dma((n_slots + 1,)),
                dma, dma, dma, dma,
            ],
            compiler_params=pltpu.CompilerParams(collective_id=0, has_side_effects=True, vmem_limit_bytes=63 << 20),
        )(hidden, ln_gain.reshape(1, width), ln_bias.reshape(1, width), embedding, targets, score_mask)
        row = jax.ShapeDtypeStruct((1, tokens), f32)
        norm, logp, seq, top = pl.pallas_call(
            finish, out_shape=(row, row, jax.ShapeDtypeStruct((1, 1), f32), row), in_specs=[vmem], out_specs=(vmem,) * 4,
        )(pltpu.with_memory_space_constraint(out, pltpu.VMEM))
        return norm, logp, seq.reshape(1), top

    row_spec = P("dp", None)
    return jax.shard_map(local_part, mesh=mesh, in_specs=(P("dp", None, None), P(), P(), P("tp", None), row_spec, row_spec), out_specs=(row_spec, row_spec, P("dp"), row_spec), check_vma=False)
```

```python
import functools

import jax
import jax.numpy as jnp
from jax import lax
from jax.experimental import pallas as pl
from jax.experimental.pallas import tpu as pltpu
from jax.sharding import PartitionSpec as P

OPT_VOCAB = 50272
LN_EPS = 1e-5
CHUNK = 512
SHARED = 5632
BLOCK = 256
HELD = 7
NORM_ROWS = 64
MESH = pl.DeviceIdType.MESH
NEG_INF = float("-inf")
NT = (((1,), (1,)), ((), ()))


def kernel(n_tp, x_hbm, gain_hbm, bias_hbm, emb_hbm, tgt_hbm, msk_hbm, out_ref,
           gain_ref, bias_ref, tgt_ref, msk_ref, x_buf, h_buf, hs_buf, fr_buf, e_buf, z_buf, zs_buf, tg_send, tg_recv, own_send, far_send, all_recv,
           in_sem, x_sem, s_sem, e_sem, hs_sem, hr_sem, rs_sem, rr_sem, ts_sem, tr_sem, ss_sem, sr_sem):
    dp, tp = lax.axis_index("dp"), lax.axis_index("tp")
    rows, width = emb_hbm.shape
    tokens = x_buf.shape[1]
    half = tokens // 2
    n_slots = width // CHUNK
    last = n_slots
    short = CHUNK // 2
    single = rows - 2 * SHARED
    per_slot = SHARED // single
    n_held = e_buf.shape[0]
    first_single = n_held - pl.cdiv(n_slots, per_slot)
    core, y, z = tp % 2, dp % 2, dp // 2
    parity = (y + z) % 2
    dp_y, dp_z = dp + 1 - 2 * y, dp + 2 - 4 * z
    dp_far = dp_y + core * (dp_z - dp_y)
    tp_other = tp + 1 - 2 * core
    first_row = tp * rows
    shared_row = pl.multiple_of(parity * SHARED, 16)
    mine = pl.ds(pl.multiple_of(core * half, half), half)
    rest = pl.ds(pl.multiple_of((1 - core) * half, half), half)

    def place(c, halves=False):
        if halves or (isinstance(c, int) and c < 2):
            lanes = pl.ds(c * short if isinstance(c, int) else pl.multiple_of(c * short, short), short)
            return 0, lanes, lanes
        start = (c - 1) * CHUNK
        return c - 1, pl.ds(0, CHUNK), pl.ds(start if isinstance(c, int) else pl.multiple_of(start, CHUNK), CHUNK)

    def fetch_x(c, part, sl):
        slot, lanes, cols = place(c)
        return pltpu.make_async_copy(x_hbm.at[0, sl, cols], x_buf.at[slot, sl, lanes], x_sem.at[part])

    def wait_x(part, sl):
        ref = x_buf.at[:, sl]
        pltpu.make_async_copy(ref, ref, x_sem.at[part]).wait()

    def single_at(slot):
        return first_single + slot // per_slot, pl.ds(pl.multiple_of(slot % per_slot * single, 16), single)

    def fetch_single(c):
        slot, lanes, cols = place(c)
        at, sl = single_at(slot)
        return pltpu.make_async_copy(emb_hbm.at[pl.ds(2 * SHARED, single), cols], e_buf.at[at, sl, lanes], s_sem.at[slot])

    def wait_single(slot):
        at, sl = single_at(slot)
        ref = e_buf.at[at, sl]
        pltpu.make_async_copy(ref, ref, s_sem.at[slot]).wait()

    def held(c):
        return n_slots - n_held if isinstance(c, int) and n_held <= c < last else c

    def fetch_shared(c, halves=False):
        slot, lanes, cols = place(c, halves)
        return pltpu.make_async_copy(emb_hbm.at[pl.ds(shared_row, SHARED), cols], e_buf.at[held(slot), :, lanes], e_sem.at[c])

    def send_h(c):
        slot, lanes, _ = place(c)
        return pltpu.make_async_remote_copy(hs_buf.at[slot, :, lanes], fr_buf.at[slot, mine, lanes], hs_sem, hr_sem.at[c], device_id={"dp": dp_far, "tp": tp}, device_id_type=MESH)

    def relay_h(c, halves=False):
        slot, lanes, _ = place(c, halves)
        ref = fr_buf.at[slot, mine, lanes]
        return pltpu.make_async_remote_copy(ref, ref, rs_sem, rr_sem.at[c], device_id={"dp": dp, "tp": tp_other}, device_id_type=MESH)

    def send_targets(k):
        to = tp if k == 0 else tp_other
        return pltpu.make_async_remote_copy(tg_send, tg_recv.at[core], ts_sem, tr_sem, device_id={"dp": dp_far, "tp": to}, device_id_type=MESH)

    small = [pltpu.make_async_copy(src, dst, in_sem.at[i]) for i, (src, dst) in enumerate(
        [(tgt_hbm, tgt_ref), (gain_hbm, gain_ref), (bias_hbm, bias_ref), (msk_hbm, msk_ref)])]
    for c in range(last + 1):
        fetch_x(c, 0, mine).start()
    for c in range(5):
        fetch_single(c).start(priority=1)
    for c in small:
        c.start()
    for c in range(last + 1):
        fetch_x(c, 1, rest).start()

    barrier = pltpu.get_barrier_semaphore()
    group = [(dp, k) for k in range(1, n_tp)] + [(dp_y, k) for k in range(n_tp)] + [(dp_z, k) for k in range(n_tp)]
    for d, k in group:
        pl.semaphore_signal(barrier, inc=1, device_id={"dp": d, "tp": (tp + k) % n_tp}, device_id_type=MESH)
    for c in small:
        c.wait()
    tg_send[...] = jnp.broadcast_to(tgt_ref[...].astype(jnp.float32), tg_send.shape)

    wait_x(0, mine)
    for c in range(5, last + 1):
        fetch_single(c).start(priority=1)
    for c in range(3):
        fetch_shared(c).start(priority=1)

    def norm_rows(row):
        sl = pl.ds(pl.multiple_of(row, NORM_ROWS), NORM_ROWS)

        def load(k):
            return x_buf[k, sl, :].astype(jnp.float32)

        def cols(ref, k):
            return ref[:, k * CHUNK:(k + 1) * CHUNK]

        mean = jnp.sum(sum(load(k) for k in range(n_slots)), axis=-1, keepdims=True) / width
        var = jnp.sum(sum((load(k) - mean) * (load(k) - mean) for k in range(n_slots)), axis=-1, keepdims=True) / width
        scale = lax.rsqrt(var + LN_EPS)
        for k in range(n_slots):
            h = ((load(k) - mean) * scale * cols(gain_ref, k) + cols(bias_ref, k)).astype(jnp.bfloat16)
            h_buf[k, sl, :] = h
            yield k, h

    def norm_sent(g, carry):
        for k, h in norm_rows(core * half + g * NORM_ROWS):
            hs_buf[k, pl.ds(pl.multiple_of(g * NORM_ROWS, NORM_ROWS), NORM_ROWS), :] = h.astype(jnp.float32)
        return carry

    def norm_kept(g, carry):
        for _ in norm_rows((1 - core) * half + g * NORM_ROWS):
            pass
        return carry

    lax.fori_loop(0, half // NORM_ROWS, norm_sent, 0)
    pl.semaphore_wait(barrier, len(group))
    for c in range(last + 1):
        send_h(c).start()
    for k in range(2):
        send_targets(k).start()
    wait_x(1, rest)
    lax.fori_loop(0, half // NORM_ROWS, norm_kept, 0)

    def single_dot(slot):
        at, sl = single_at(slot)
        return lax.dot_general(e_buf[at, sl, :], h_buf[slot, 0:tokens, :], NT, preferred_element_type=jnp.float32)

    zs_buf[...] = jnp.zeros_like(zs_buf)

    def single_step(i, carry):
        @pl.when(i == 2)
        def _():
            fetch_shared(3).start(priority=1)

        @pl.when(i == 3)
        def _():
            send_h(0).wait_recv()
            relay_h(0).start()
        for k in range(2):
            wait_single(2 * i + k)
        zs_buf[...] += single_dot(2 * i) + single_dot(2 * i + 1)
        return carry

    lax.fori_loop(0, n_slots // 2, single_step, 0)

    sub = lax.broadcasted_iota(jnp.int32, (8, 1), 0)
    lane = lax.broadcasted_iota(jnp.int32, (1, tokens), 1)

    def online(z, start, target, state, limit=None):
        n_rows, lanes = z.shape
        z = z.reshape(n_rows // 8, 8, lanes)
        step = lax.broadcasted_iota(jnp.int32, z.shape, 0) * 8
        if limit is not None:
            z = jnp.where(step < (limit - start) - sub[None], z, NEG_INF)
        t8 = jnp.sum(jnp.where(step == (target - start - sub)[None], z, 0.0), axis=0)
        m8 = jnp.max(z, axis=0)
        if state is None:
            return m8, jnp.sum(jnp.exp(z - m8[None]), axis=0), t8
        m_new = jnp.maximum(state[0], m8)
        s8 = state[1] * jnp.exp(state[0] - m_new) + jnp.sum(jnp.exp(z - m_new[None]), axis=0)
        return m_new, s8, state[2] + t8

    def fold(state):
        m1 = jnp.max(state[0], axis=0, keepdims=True)
        return m1, jnp.sum(state[1] * jnp.exp(state[0] - m1), axis=0, keepdims=True), jnp.sum(state[2], axis=0, keepdims=True)

    def pass_on(c):
        send_h(c).wait_recv()
        relay_h(c).start()

    def shared_ready(c, halves=False):
        fetch_shared(c, halves).wait()
        if isinstance(c, int):
            if c + 1 <= last:
                pass_on(c + 1)
            if c + 4 <= last:
                fetch_shared(c + 4).start(priority=1)
        elif halves:
            pass_on(2)
            fetch_shared(5).start(priority=1)
        else:
            pass_on(c + 1)

            @pl.when(c + 4 < n_held)
            def _():
                fetch_shared(c + 4).start(priority=1)

            for k in range(n_held, last + 1):
                @pl.when(c + 4 == k)
                def _():
                    fetch_shared(k).start(priority=1)
        relay_h(c, halves).wait_recv()
        slot, lanes, _ = place(c, halves)
        h_buf[slot, tokens:2 * tokens, lanes] = fr_buf[slot, :, lanes].astype(jnp.bfloat16)

    def shared_dot(c, sl, halves=False):
        slot, lanes, _ = place(c, halves)
        return lax.dot_general(e_buf[held(slot), sl, lanes], h_buf[slot, :, lanes], NT, preferred_element_type=jnp.float32)

    target = tgt_ref[...]
    every = pl.ds(0, SHARED)
    shared_ready(0)
    z_buf[...] = shared_dot(0, every)
    m_s, s_s, t_s = fold(online(zs_buf[...], first_row + 2 * SHARED, target, None, OPT_VOCAB))

    def shared_chunk(c, carry):
        shared_ready(c)
        z_buf[...] += shared_dot(c, every)
        return carry

    def second_half(c, carry):
        shared_ready(c, True)
        z_buf[...] += shared_dot(c, every, True)
        return carry

    lax.fori_loop(1, 2 + dp // 1024, second_half, 0)
    lax.fori_loop(2, last, shared_chunk, 0)
    shared_ready(last)
    z_buf[...] += shared_dot(last, every)

    pltpu.make_async_remote_copy(tg_recv, tg_recv, ts_sem, tr_sem, device_id={"dp": dp_far, "tp": tp}, device_id_type=MESH).wait_recv()
    far_target = jnp.where(lane < half, tg_recv[0, 0:1, :], tg_recv[1, 0:1, :]).astype(jnp.int32)
    n_blocks = SHARED // BLOCK

    def shared_stats(first_lane, target):
        def block(i):
            return z_buf[pl.ds(pl.multiple_of(i * BLOCK, BLOCK), BLOCK), first_lane:first_lane + tokens].reshape(BLOCK // 8, 8, tokens)

        def add(i, m8, s8, t8):
            zz = block(i)
            step = lax.broadcasted_iota(jnp.int32, zz.shape, 0) * 8
            t8 = t8 + jnp.sum(jnp.where(step == (target - (first_row + shared_row + i * BLOCK) - sub)[None], zz, 0.0), axis=0)
            return s8 + jnp.sum(jnp.exp(zz - m8[None]), axis=0), t8

        def step(i, state):
            m8, s8, t8 = state
            m_new = jnp.maximum(m8, jnp.max(block(i + 1), axis=0))
            s8, t8 = add(i, m8, s8, t8)
            return m_new, s8 * jnp.exp(m8 - m_new), t8

        zero = jnp.zeros((8, tokens), jnp.float32)
        m8, s8, t8 = lax.fori_loop(0, n_blocks - 1, step, (jnp.max(block(0), axis=0), zero, zero))
        return fold((m8, *add(n_blocks - 1, m8, s8, t8)))

    def send_stats(src, first, end):
        for i, (d, k) in list(enumerate(group))[first:end]:
            slot = k - 1 if i < n_tp - 1 else (n_tp - 1 + k if i < 2 * n_tp - 1 else 2 * n_tp - 1 + k)
            pltpu.make_async_remote_copy(src, all_recv.at[slot], ss_sem, sr_sem, device_id={"dp": d, "tp": (tp + k) % n_tp}, device_id_type=MESH).start()

    for j, v in enumerate(shared_stats(tokens, far_target)):
        far_send[j:j + 1, :] = v
    send_stats(far_send, n_tp - 1, len(group))
    m_h, s_h, t_h = shared_stats(0, target)
    m_o = jnp.maximum(m_s, m_h)
    s_o = s_s * jnp.exp(m_s - m_o) + s_h * jnp.exp(m_h - m_o)
    t_o = t_s + t_h
    for j, v in enumerate((m_o, s_o, t_o)):
        own_send[j:j + 1, :] = v
    send_stats(own_send, 0, n_tp - 1)

    def total_of(ref, send_sem, recv_sem):
        return pltpu.make_async_remote_copy(ref, ref, send_sem, recv_sem, device_id={"dp": dp, "tp": tp_other}, device_id_type=MESH)

    total_of(hs_buf, hs_sem, sr_sem).wait_send()
    total_of(hs_buf, rs_sem, sr_sem).wait_send()
    total_of(tg_recv, ts_sem, sr_sem).wait_send()
    total_of(all_recv, ss_sem, sr_sem).wait_recv()

    parts = [(m_o, s_o, t_o)]
    for k in range(n_tp - 1):
        parts.append(tuple(all_recv[k, j:j + 1, :] for j in range(3)))
    for k in range(n_tp - 1, 2 * n_tp - 1):
        parts.append(tuple(jnp.where(lane < half, all_recv[k, j:j + 1, :], all_recv[k + n_tp, j:j + 1, :]) for j in range(3)))
    m = functools.reduce(jnp.maximum, [p[0] for p in parts])
    total = sum(p[1] * jnp.exp(p[0] - m) for p in parts)
    z_t = sum(p[2] for p in parts)
    norm = m + jnp.log(total)
    logp = (z_t - norm) * msk_ref[...].astype(jnp.float32)
    out_ref[0:1, :] = norm
    out_ref[1:2, :] = logp
    out_ref[2:3, :] = m - norm
    total_of(all_recv, ss_sem, sr_sem).wait_send()


def finish(all_ref, norm_ref, logp_ref, seq_ref, top_ref):
    logp = all_ref[1:2, :]
    norm_ref[...] = all_ref[0:1, :]
    logp_ref[...] = logp
    top_ref[...] = all_ref[2:3, :]
    seq_ref[...] = jnp.sum(logp, axis=-1, keepdims=True)


def solution(mesh):
    n_tp = mesh.shape["tp"]

    def local_part(hidden, ln_gain, ln_bias, embedding, targets, score_mask):
        _, tokens, width = hidden.shape
        rows = embedding.shape[0]
        n_slots = width // CHUNK
        single = rows - 2 * SHARED
        vmem = pl.BlockSpec(memory_space=pltpu.VMEM)
        hbm = pl.BlockSpec(memory_space=pl.ANY)
        f32, bf16 = jnp.float32, jnp.bfloat16
        dma = pltpu.SemaphoreType.DMA
        n_group = 3 * n_tp - 1
        out = pl.pallas_call(
            functools.partial(kernel, n_tp),
            out_shape=pltpu.VMEM((8, tokens), f32),
            in_specs=[hbm] * 6,
            out_specs=vmem,
            scratch_shapes=[
                pltpu.VMEM((1, width), f32),
                pltpu.VMEM((1, width), f32),
                pltpu.VMEM((1, tokens), jnp.int32),
                pltpu.VMEM((1, tokens), jnp.int32),
                pltpu.VMEM((n_slots, tokens, CHUNK), bf16),
                pltpu.VMEM((n_slots, 2 * tokens, CHUNK), bf16),
                pltpu.VMEM((n_slots, tokens // 2, CHUNK), f32),
                pltpu.VMEM((n_slots, tokens, CHUNK), f32),
                pltpu.VMEM((HELD, SHARED, CHUNK), bf16),
                pltpu.VMEM((SHARED, 2 * tokens), f32),
                pltpu.VMEM((single, tokens), f32),
                pltpu.VMEM((8, tokens), f32),
                pltpu.VMEM((2, 8, tokens), f32),
                pltpu.VMEM((8, tokens), f32),
                pltpu.VMEM((8, tokens), f32),
                pltpu.VMEM((n_group, 8, tokens), f32),
                dma((4,)), dma((2,)), dma((n_slots,)), dma((n_slots + 1,)), dma, dma((n_slots + 1,)), dma, dma((n_slots + 1,)),
                dma, dma, dma, dma,
            ],
            compiler_params=pltpu.CompilerParams(collective_id=0, has_side_effects=True, vmem_limit_bytes=63 << 20),
        )(hidden, ln_gain.reshape(1, width), ln_bias.reshape(1, width), embedding, targets, score_mask)
        row = jax.ShapeDtypeStruct((1, tokens), f32)
        norm, logp, seq, top = pl.pallas_call(
            finish, out_shape=(row, row, jax.ShapeDtypeStruct((1, 1), f32), row), in_specs=[vmem], out_specs=(vmem,) * 4,
        )(pltpu.with_memory_space_constraint(out, pltpu.VMEM))
        return norm, logp, seq.reshape(1), top

    row_spec = P("dp", None)
    return jax.shard_map(local_part, mesh=mesh, in_specs=(P("dp", None, None), P(), P(), P("tp", None), row_spec, row_spec), out_specs=(row_spec, row_spec, P("dp"), row_spec), check_vma=False)
```
